128 devices in a mesh: rows: 64 (over y_lo, x, z, core), chan: 2 (over y_hi).
Axes of the slice: x: 4, y: 4 (y_hi: 2, y_lo: 2; y = y_hi * 2 + y_lo), z: 4, core: 2. Of those that a mesh axis runs over, the one named last changes fastest.
Arguments:
- pixels: float32 [4096, 16384], P(('chan', 'rows')), parts along dimension 0, may hold values from -6 to 6
- row_taps: float32 [32768], P(('chan', 'rows')), parts along dimension 0, may hold values from -0.046875 to 0.046875
- column_taps: float32 [4096], P(('chan', 'rows')), parts along dimension 0, may hold values from -0.125 to 0.125
- stencil: float32 [6, 3], P('chan'), parts along dimension 0, may hold values from -3 to 3
Outputs:
- filtered: float32 [4096, 16384], P(('chan', 'rows')), parts along dimension 0
The draws below stay inside these ranges and needn't reach their ends.
There are 2 independent parts, one for each index of `chan`. The reference program is written for one: setup_inputs(seed, part) draws one part's arguments, and reference() takes and returns one part's arrays. A program takes and returns all parts, laid end to end along the dimension named above; each array names one. Nothing has to cross between parts.
All inputs are finite; a program needn't handle non-finite values.
Results may differ from the reference program's by a relative error of at most 0.0003.
Values sent between devices are 32-bit elements; how exact they have to be, the bound alone decides.
A program may use at most 128 MiB of HBM per device.

```python
import jax
import jax.numpy as jnp

NX = 16384
NY = 2048


def steps_of(key, dims, shards, least, largest):
    def one(position, parts):
        heights = jax.random.uniform(jax.random.fold_in(jax.random.fold_in(key, 6), position), (parts,), jnp.float32, least / len(shards), largest / len(shards))
        return jnp.repeat(jnp.exp(heights), dims[position] // parts).reshape((-1,) + (1,) * (len(dims) - position - 1))

    loudness = one(*shards[0])
    for cut in shards[1:]:
        loudness = loudness * one(*cut)
    return loudness


def bell_draw(key, dims, scale, limit, pieces=(), kind=jnp.bfloat16):
    loudness = steps_of(key, dims, pieces, -0.22, 0.18) if pieces else 1.0
    values = jax.random.normal(key, dims, jnp.float32) * scale * loudness
    return jnp.minimum(jnp.maximum(values, -limit), limit).astype(kind)


def setup_inputs(seed: int = 0, part: int = 0) -> dict:
    streams_of = jax.random.split(jax.random.key(seed), 5)
    part_keys = jax.random.split(jax.random.fold_in(streams_of[4], part), 5)
    return {
        "pixels": bell_draw(part_keys[0], (NY, NX), 1.0, 6.0, ((0, 64),), jnp.float32),
        "row_taps": bell_draw(part_keys[1], (NX,), NX ** -0.5, 0.046875, ((0, 64),), jnp.float32),
        "column_taps": bell_draw(part_keys[2], (NY,), NY ** -0.5, 0.125, ((0, 64),), jnp.float32),
        "stencil": bell_draw(part_keys[3], (3, 3), 0.5, 3.0, (), jnp.float32),
    }


def reference(pixels, row_taps, column_taps, stencil):
    row_spectrum = jnp.fft.rfft(row_taps)
    column_spectrum = jnp.fft.rfft(column_taps)
    row_done = jnp.fft.irfft(jnp.fft.rfft(pixels, axis=1) * row_spectrum[None, :], n=NX, axis=1)
    combined = jnp.fft.irfft(jnp.fft.rfft(row_done, axis=0) * column_spectrum[:, None], n=NY, axis=0)
    filtered = combined.astype(pixels.dtype)
    for offset_row in range(3):
        for offset_col in range(3):
            moved = jnp.roll(pixels, (1 - offset_row, 1 - offset_col), axis=(0, 1))
            filtered = filtered + stencil[offset_row, offset_col] * moved
    return filtered
```

```python
import functools
import math

import jax
import jax.numpy as jnp
import ml_dtypes
import numpy as np
from jax import lax
from jax.experimental import pallas as pl
from jax.experimental.pallas import tpu as pltpu
from jax.sharding import PartitionSpec as P

MESH = pl.DeviceIdType.MESH
F32, BF16 = jnp.float32, jnp.bfloat16
PEERS = 64
LANES = 128
BLOCKS = 16
GROUP = 7


def split_np(values):
    high = values.astype(ml_dtypes.bfloat16)
    low = (values - high.astype(np.float64)).astype(ml_dtypes.bfloat16)
    return high, low


def plane_tables():
    pos = np.arange(LANES)
    fwd = np.zeros((LANES, LANES))
    inv = np.zeros((LANES, LANES))
    for s in range(PEERS):
        angle = 2 * np.pi * (pos * s % LANES) / LANES
        if s == 0:
            fwd[0], fwd[1] = 1.0, (-1.0) ** pos
            inv[:, 0], inv[:, 1] = 1.0 / LANES, (-1.0) ** pos / LANES
        else:
            fwd[2 * s], fwd[2 * s + 1] = np.cos(angle), -np.sin(angle)
            inv[:, 2 * s], inv[:, 2 * s + 1] = 2 * np.cos(angle) / LANES, -2 * np.sin(angle) / LANES
    stacked = []
    for table in (fwd, inv):
        high, low = split_np(table)
        stacked.append(np.block([[high, high], [low, low]]))
    return stacked


def tap_tables():
    tab = np.zeros((PEERS, 8, 2 * LANES), np.float64)
    pos = np.arange(LANES)
    cols = 4 * (pos // 2) + pos % 2
    for s in range(PEERS):
        for row, freq in ((0, s), (2, s if s else LANES // 2)):
            angle = 2 * np.pi * (pos * freq % LANES) / LANES
            tab[s, row, cols], tab[s, row + 1, cols] = np.cos(angle), -np.sin(angle)
            turn = 2 * np.pi * freq / LANES
            tab[s, 4 + row], tab[s, 5 + row] = np.cos(turn), -np.sin(turn)
    return tab.astype(np.float32)


def turned(k, n, re, im, sign):
    angle = 2 * math.pi * k / n
    c, s = math.cos(angle), sign * math.sin(angle)
    if k == 0:
        return re, im
    if 4 * k == n:
        return (-im, re) if sign > 0 else (im, -re)
    if 8 * k == n:
        return (re - s / abs(s) * im) * c, (im + s / abs(s) * re) * c
    return re * c - im * s, re * s + im * c


def rfft(values):
    n = len(values)
    if n == 2:
        return [(values[0] + values[1], None), (values[0] - values[1], None)]
    even, odd = rfft(values[0::2]), rfft(values[1::2])
    out = [None] * (n // 2 + 1)
    for k in range(n // 4 + 1):
        er, ei = even[k]
        orr, oi = odd[k]
        if k == 0:
            out[0], out[n // 2] = (er + orr, None), (er - orr, None)
        elif 4 * k == n:
            out[k] = (er, -orr)
        else:
            tr, ti = turned(k, n, orr, oi, -1)
            out[k] = (er + tr, ei + ti)
            out[n // 2 - k] = (er - tr, ti - ei)
    return out


def irfft(spectrum):
    n = 2 * (len(spectrum) - 1)
    if n == 2:
        a, b = spectrum[0][0], spectrum[1][0]
        return [a + b, a - b]
    even, odd = [None] * (n // 4 + 1), [None] * (n // 4 + 1)
    for k in range(n // 4 + 1):
        ar, ai = spectrum[k]
        br, bi = spectrum[n // 2 - k]
        if k == 0:
            even[0], odd[0] = (ar + br, None), (ar - br, None)
        elif 4 * k == n:
            even[k], odd[k] = (2.0 * ar, None), (-2.0 * ai, None)
        else:
            even[k] = (ar + br, ai - bi)
            odd[k] = turned(k, n, ar - br, ai + bi, +1)
    out = [None] * n
    out[0::2], out[1::2] = irfft(even), irfft(odd)
    return out


def halves(value):
    high = value.astype(BF16)
    return high, (value - high.astype(F32)).astype(BF16)


def toeplitz(line):
    wide = jnp.broadcast_to(line, (LANES, 2 * LANES))
    return pltpu.roll(wide, 0, 1, stride=1, stride_axis=0)[:, :LANES]


def plane_step(table_ref, src, offset, dst, extra=None):
    def step(i, _):
        pair = jnp.concatenate([src[offset + 2 * i], src[offset + 2 * i + 1]], axis=1)
        out = jnp.dot(table_ref[...], jnp.concatenate(halves(pair), axis=0), preferred_element_type=F32)
        out = out[:LANES] + out[LANES:]
        one, two = out[:, :LANES], out[:, LANES:]
        if extra is not None:
            one, two = one + extra[2 * i], two + extra[2 * i + 1]
        dst[2 * i], dst[2 * i + 1] = one, two
        return 0

    lax.fori_loop(0, 16, step, 0, unroll=2)


def kernel(
    x_hbm, row_taps, col_taps, stencil, tab_hbm, fwd_ref, inv_ref, out_hbm,
    xs, planes, got, back, sent, local, taps, my_taps, tab, lines, blocks, left, spec, prod, high, low, right,
    in_sem, out_sem, tab_sem, tap_send, tap_recv, halo_send, halo_recv, a_send, a_recv, b_send, b_recv,
):
    me = lax.axis_index("rows")

    def load(p, _):
        pltpu.make_async_copy(
            x_hbm.at[:, pl.ds(pl.multiple_of(p * LANES, LANES), LANES)], xs.at[pl.ds(1, 32), p, :], in_sem
        ).start()
        return 0

    lax.fori_loop(0, LANES, load, 0, unroll=8)
    tab_copy = pltpu.make_async_copy(tab_hbm.at[me], tab, tab_sem)
    tab_copy.start()

    barrier = pltpu.get_barrier_semaphore()

    def peer(i):
        k = (i * (i + 1) // 2) % PEERS
        core, z, x, y = k % 2, (k // 2) % 4, (k // 8) % 4, k // 32
        return (
            ((me // 32 + y) % 2 * 4 + (me // 8 + x) % 4) * 4 + (me // 2 + z) % 4
        ) * 2 + (me + core) % 2

    def greet(i, _):
        pl.semaphore_signal(barrier, inc=1, device_id={"rows": (me + i) % PEERS}, device_id_type=MESH)
        return 0

    lax.fori_loop(1, PEERS, greet, 0)

    my_taps[0:1, :] = row_taps[0:128].reshape(1, LANES)
    my_taps[1:2, :] = row_taps[128:256].reshape(1, LANES)
    padded = jnp.concatenate([col_taps[...].reshape(1, 32), jnp.zeros((1, 96), F32)], axis=1)
    my_taps[2:3, :] = pltpu.roll(padded, (me % 4) * 32, 1)
    my_taps[3:4, :] = jnp.zeros((1, LANES), F32)

    pltpu.make_async_copy(xs.at[pl.ds(1, 32)], xs.at[pl.ds(1, 32)], in_sem).wait()
    plane_step(fwd_ref, xs, 1, planes)
    pl.semaphore_wait(barrier, PEERS - 1)

    def remote(src, dst, send, recv, to):
        return pltpu.make_async_remote_copy(
            src_ref=src, dst_ref=dst, send_sem=send, recv_sem=recv, device_id={"rows": to}, device_id_type=MESH
        )

    def send_taps(i, _):
        remote(my_taps, taps.at[pl.ds(pl.multiple_of(me * 4, 4), 4), :], tap_send, tap_recv, peer(i)).start()
        return 0

    lax.fori_loop(1, PEERS, send_taps, 0)
    down = remote(xs.at[32], xs.at[0], halo_send.at[0], halo_recv.at[0], (me + 1) % PEERS)
    up = remote(xs.at[1], xs.at[33], halo_send.at[1], halo_recv.at[1], (me + PEERS - 1) % PEERS)
    down.start()
    up.start()

    for c in range(2):

        def send_plane(i, _):
            to = peer(i)
            remote(
                planes.at[:, 2 * to + c, :],
                got.at[c, pl.ds(pl.multiple_of(me * 32, 32), 32)],
                a_send.at[c],
                a_recv.at[c],
                to,
            ).start()
            return 0

        lax.fori_loop(1, PEERS, send_plane, 0)

    for c in range(2):

        def own(r, _):
            got[c, pl.ds(me * 32 + r, 1), :] = planes[r, pl.ds(2 * me + c, 1), :]
            return 0

        lax.fori_loop(0, 32, own, 0)

    taps[pl.ds(pl.multiple_of(me * 4, 4), 4), :] = my_taps[...]
    tab_copy.wait()
    pltpu.make_async_copy(taps.at[pl.ds(0, 252)], taps.at[pl.ds(0, 252)], tap_recv).wait()
    g = jnp.dot(tab[...], taps[...], preferred_element_type=F32, precision=lax.Precision.HIGHEST)
    gr, gi, hr, hi = g[0:1], g[1:2], g[2:3], g[3:4]
    wr, wi, vr, vi = (tab[i : i + 1, 0:LANES] for i in (4, 5, 6, 7))
    real = toeplitz(jnp.concatenate([gr, wr * gr - wi * gi], axis=1))
    imag = toeplitz(jnp.concatenate([gi, wr * gi + wi * gr], axis=1))
    real_two = toeplitz(jnp.concatenate([hr, vr * hr - vi * hi], axis=1))
    for r, c, value in ((0, 0, real), (0, 1, imag), (1, 0, -imag), (1, 1, real_two)):
        rows, cols = pl.ds(r * LANES, LANES), c * LANES
        h, l = halves(value)
        right[rows, cols : cols + LANES] = h
        right[rows, 256 + cols : 256 + cols + LANES] = l

    lines[...] = sum(taps[pl.ds(4 * e + 2, BLOCKS, stride=16), :] for e in range(4))

    def block(d, _):
        line = jnp.concatenate([lines[pl.ds(d, 1), :], lines[pl.ds((d + BLOCKS - 1) % BLOCKS, 1), :]], axis=1)
        blocks[d] = toeplitz(line).T
        return 0

    lax.fori_loop(0, BLOCKS, block, 0)

    def block_spectrum(t, _):
        rows = pl.ds(pl.multiple_of(t * 16, 16), 16)
        freqs = rfft([blocks[d, rows, :] for d in range(BLOCKS)])
        zero = jnp.zeros((16, LANES), F32)
        for f in range(8):
            if f == 0:
                quads = ((freqs[0][0], zero), (zero, freqs[8][0]))
            else:
                quads = ((freqs[f][0], -freqs[f][1]), (freqs[f][1], freqs[f][0]))
            for r in range(2):
                for c in range(2):
                    h, l = halves(quads[r][c] * (1.0 / BLOCKS))
                    cols = slice(c * LANES, (c + 1) * LANES)
                    left[f, pl.ds(pl.multiple_of(r * LANES + t * 16, 16), 16), cols] = h
                    left[f, pl.ds(pl.multiple_of(256 + r * LANES + t * 16, 16), 16), cols] = l
        return 0

    lax.fori_loop(0, 8, block_spectrum, 0)

    down.wait()
    up.wait()
    lane = lax.broadcasted_iota(jnp.int32, (LANES, LANES), 1)

    def stencil_row(y, _):
        total = jnp.zeros((LANES, LANES), F32)
        for a in range(3):
            here = xs[y + a]
            before, after = pltpu.roll(here, 1, 1), pltpu.roll(here, LANES - 1, 1)
            before = jnp.where(lane == 0, pltpu.roll(before, 1, 0), before)
            after = jnp.where(lane == LANES - 1, pltpu.roll(after, LANES - 1, 0), after)
            total = total + stencil[a, 0] * before + stencil[a, 1] * here + stencil[a, 2] * after
        local[y] = total
        return 0

    lax.fori_loop(0, 32, stencil_row, 0)

    for c in range(2):
        pltpu.make_async_copy(got.at[c, pl.ds(0, 2016)], got.at[c, pl.ds(0, 2016)], a_recv.at[c]).wait()

        def spectrum(t, _):
            freqs = rfft(
                [got[c, pl.ds(pl.multiple_of(b * LANES + t * 16, 16), 16), :] for b in range(BLOCKS)]
            )
            for f in range(8):
                pair = (freqs[0][0], freqs[8][0]) if f == 0 else freqs[f]
                for r in range(2):
                    h, l = halves(pair[r])
                    rows = pl.ds(pl.multiple_of(r * LANES + t * 16, 16), 16)
                    spec[f, rows, 0:LANES] = h
                    spec[f, rows, LANES : 2 * LANES] = l
            return 0

        lax.fori_loop(0, 8, spectrum, 0)

        def multiply(f, _):
            out = jnp.dot(left[f], spec[f], preferred_element_type=F32)
            out = out[:256] + out[256:]
            prod[f] = out[:, :LANES] + out[:, LANES:]
            return 0

        lax.fori_loop(0, 8, multiply, 0)

        def unspectrum(t, _):
            freqs = []
            for f in range(9):
                re = prod[f % 8, pl.ds(pl.multiple_of((f // 8) * LANES + t * 16, 16), 16), :]
                im = None
                if f % 8:
                    im = prod[f, pl.ds(pl.multiple_of(LANES + t * 16, 16), 16), :]
                freqs.append((re, im))
            for b, value in enumerate(irfft(freqs)):
                rows = pl.ds(pl.multiple_of(b * LANES + t * 16, 16), 16)
                high[rows, c * LANES : (c + 1) * LANES], low[rows, c * LANES : (c + 1) * LANES] = halves(value)
            return 0

        lax.fori_loop(0, 8, unspectrum, 0)

    def product(owners):
        rows = [pl.ds(pl.multiple_of(t * 32, 32), 32) for t in owners]
        hs = jnp.concatenate([high[r, :] for r in rows], axis=0)
        ls = jnp.concatenate([low[r, :] for r in rows], axis=0)
        return (
            jnp.dot(hs, right[:, 0:256], preferred_element_type=F32)
            + jnp.dot(hs, right[:, 256:512], preferred_element_type=F32)
            + jnp.dot(ls, right[:, 0:256], preferred_element_type=F32)
        )

    def send_back(j, _):
        owners = [peer(j * GROUP + 1 + k) for k in range(GROUP)]
        out = product(owners)
        for k, to in enumerate(owners):
            rows = pl.ds(pl.multiple_of(to * 32, 32), 32)
            for c in range(2):
                sent[c, rows, :] = out[k * 32 : (k + 1) * 32, c * LANES : (c + 1) * LANES]
                remote(sent.at[c, rows], back.at[:, 2 * me + c, :], b_send, b_recv, to).start()
        return 0

    lax.fori_loop(0, (PEERS - 1) // GROUP, send_back, 0)
    mine = product([me])
    for c in range(2):
        for r in range(32):
            back[r, pl.ds(2 * me + c, 1), :] = mine[r : r + 1, c * LANES : (c + 1) * LANES]

    for c in range(2):
        pltpu.make_async_copy(got.at[c, pl.ds(0, 2016)], got.at[c, pl.ds(0, 2016)], a_send.at[c]).wait()
    pltpu.make_async_copy(taps.at[pl.ds(0, 252)], taps.at[pl.ds(0, 252)], tap_send).wait()
    pltpu.make_async_copy(back.at[:, pl.ds(0, 126)], back.at[:, pl.ds(0, 126)], b_recv).wait()
    plane_step(inv_ref, back, 0, planes, local)

    def store(p, _):
        pltpu.make_async_copy(
            planes.at[:, p, :], out_hbm.at[:, pl.ds(pl.multiple_of(p * LANES, LANES), LANES)], out_sem
        ).start()
        return 0

    lax.fori_loop(0, LANES, store, 0, unroll=8)
    pltpu.make_async_copy(back.at[:, pl.ds(0, 126)], back.at[:, pl.ds(0, 126)], b_send).wait()
    pltpu.make_async_copy(planes, planes, out_sem).wait()


def body(pixels, row_taps, column_taps, stencil):
    fwd, inv = plane_tables()
    vmem, anywhere = pl.BlockSpec(memory_space=pltpu.VMEM), pl.BlockSpec(memory_space=pl.ANY)
    block = (32, LANES, LANES)
    dma = pltpu.SemaphoreType.DMA
    return pl.pallas_call(
        kernel,
        out_shape=jax.ShapeDtypeStruct(pixels.shape, F32),
        in_specs=[
            anywhere, vmem, vmem, pl.BlockSpec(memory_space=pltpu.SMEM), anywhere, vmem, vmem,
        ],
        out_specs=anywhere,
        scratch_shapes=[
            pltpu.VMEM((34, LANES, LANES), F32),
            pltpu.VMEM(block, F32),
            pltpu.VMEM((2, 2048, LANES), F32),
            pltpu.VMEM(block, F32),
            pltpu.VMEM((2, 2048, LANES), F32),
            pltpu.VMEM(block, F32),
            pltpu.VMEM((4 * PEERS, LANES), F32),
            pltpu.VMEM((4, LANES), F32),
            pltpu.VMEM((8, 2 * LANES), F32),
            pltpu.VMEM((BLOCKS, LANES), F32),
            pltpu.VMEM((BLOCKS, LANES, LANES), F32),
            pltpu.VMEM((8, 512, 256), BF16),
            pltpu.VMEM((8, 256, 256), BF16),
            pltpu.VMEM((8, 256, LANES), F32),
            pltpu.VMEM((2048, 256), BF16),
            pltpu.VMEM((2048, 256), BF16),
            pltpu.VMEM((256, 512), BF16),
            dma, dma, dma, dma, dma, dma((2,)), dma((2,)), dma((2,)), dma((2,)), dma, dma,
        ],
        compiler_params=pltpu.CompilerParams(
            collective_id=0, has_side_effects=True, vmem_limit_bytes=48 * 2**20
        ),
        name="filter_rows_and_columns",
    )(pixels, row_taps, column_taps, stencil, jnp.asarray(tap_tables()), jnp.asarray(fwd), jnp.asarray(inv))


def solution(mesh):
    in_specs = (
        P(("chan", "rows"), None),
        P(("chan", "rows")),
        P(("chan", "rows")),
        P("chan", None),
    )
    return jax.shard_map(
        body, mesh=mesh, in_specs=in_specs, out_specs=P(("chan", "rows"), None), check_vma=False
    )
```

```python
import math

import jax
import jax.numpy as jnp
import ml_dtypes
import numpy as np
from jax import lax
from jax.experimental import pallas as pl
from jax.experimental.pallas import tpu as pltpu
from jax.sharding import PartitionSpec as P

MESH = pl.DeviceIdType.MESH
F32, BF16 = jnp.float32, jnp.bfloat16
PEERS = 64
LANES = 128
BLOCKS = 16
GROUP = 7


def split_np(values):
    high = values.astype(ml_dtypes.bfloat16)
    low = (values - high.astype(np.float64)).astype(ml_dtypes.bfloat16)
    return high, low


def frequency(device, phase):
    return LANES // 2 if device == 1 and phase == 0 else 2 * (device // 2) + phase


def plane_tables():
    pos = np.arange(LANES)
    fwd = np.zeros((2, PEERS, LANES))
    inv = np.zeros((2, LANES, PEERS))
    for phase in range(2):
        for device in range(PEERS):
            freq = frequency(device, phase)
            angle = 2 * np.pi * (pos * freq % LANES) / LANES
            real = freq in (0, LANES // 2)
            wave = -np.sin(angle) if device % 2 and not real else np.cos(angle)
            fwd[phase, device] = wave
            inv[phase, :, device] = wave * (1 if real else 2) / LANES
    high, low = split_np(fwd.reshape(LANES, LANES))
    forward = np.block([[high, high], [low, low]])
    high, low = split_np(inv)
    return forward, np.concatenate([high, high, low], axis=2)


def tap_tables():
    tab = np.zeros((PEERS, 8, 2 * LANES), np.float64)
    pos = np.arange(LANES)
    cols = pos // 2 % 2 * LANES + pos // 4 * 4 + pos % 2
    for device in range(PEERS):
        for phase in range(2):
            freq = frequency(device, phase)
            angle = 2 * np.pi * (pos * freq % LANES) / LANES
            tab[device, 2 * phase, cols], tab[device, 2 * phase + 1, cols] = np.cos(angle), -np.sin(angle)
            turn = 2 * np.pi * freq / LANES
            tab[device, 4 + 2 * phase], tab[device, 5 + 2 * phase] = np.cos(turn), -np.sin(turn)
    return tab.astype(np.float32)


def turned(k, n, re, im, sign):
    angle = 2 * math.pi * k / n
    c, s = math.cos(angle), sign * math.sin(angle)
    if k == 0:
        return re, im
    if 4 * k == n:
        return (-im, re) if sign > 0 else (im, -re)
    if 8 * k == n:
        return (re - s / abs(s) * im) * c, (im + s / abs(s) * re) * c
    return re * c - im * s, re * s + im * c


def rfft(values):
    n = len(values)
    if n == 2:
        return [(values[0] + values[1], None), (values[0] - values[1], None)]
    even, odd = rfft(values[0::2]), rfft(values[1::2])
    out = [None] * (n // 2 + 1)
    for k in range(n // 4 + 1):
        er, ei = even[k]
        orr, oi = odd[k]
        if k == 0:
            out[0], out[n // 2] = (er + orr, None), (er - orr, None)
        elif 4 * k == n:
            out[k] = (er, -orr)
        else:
            tr, ti = turned(k, n, orr, oi, -1)
            out[k] = (er + tr, ei + ti)
            out[n // 2 - k] = (er - tr, ti - ei)
    return out


def irfft(spectrum):
    n = 2 * (len(spectrum) - 1)
    if n == 2:
        a, b = spectrum[0][0], spectrum[1][0]
        return [a + b, a - b]
    even, odd = [None] * (n // 4 + 1), [None] * (n // 4 + 1)
    for k in range(n // 4 + 1):
        ar, ai = spectrum[k]
        br, bi = spectrum[n // 2 - k]
        if k == 0:
            even[0], odd[0] = (ar + br, None), (ar - br, None)
        elif 4 * k == n:
            even[k], odd[k] = (2.0 * ar, None), (-2.0 * ai, None)
        else:
            even[k] = (ar + br, ai - bi)
            odd[k] = turned(k, n, ar - br, ai + bi, +1)
    out = [None] * n
    out[0::2], out[1::2] = irfft(even), irfft(odd)
    return out


def halves(value):
    high = value.astype(BF16)
    return high, (value - high.astype(F32)).astype(BF16)


def toeplitz(line):
    wide = jnp.broadcast_to(line, (LANES, 2 * LANES))
    return pltpu.roll(wide, 0, 1, stride=1, stride_axis=0)[:, :LANES]


def kernel(
    x_hbm, row_taps_hbm, col_taps_hbm, stencil_hbm, tab_hbm, fwd_hbm, inv_hbm, out_hbm,
    row_taps, col_taps, stencil, fwd_ref, inv_ref, tab, my_taps, taps,
    xs, planes, got, done, other, sent, back, local, lines, blocks, left, spec, prod, right,
    in_sem, out_sem, small_sems, tap_send, tap_recv, share_send, share_recv, halo_send, halo_recv,
    a_send, a_recv, swap_send, swap_recv, b_send, b_recv,
):
    me = lax.axis_index("rows")
    core, chip = me % 2, me // 2
    sibling = chip * 2 + 1 - core

    def load(p, _):
        pltpu.make_async_copy(
            x_hbm.at[:, pl.ds(pl.multiple_of(p * LANES, LANES), LANES)], xs.at[pl.ds(1, 32), p, :], in_sem
        ).start()
        return 0

    lax.fori_loop(0, LANES, load, 0, unroll=8)
    pairs = (
        (row_taps_hbm, row_taps), (col_taps_hbm, col_taps), (stencil_hbm, stencil), (fwd_hbm, fwd_ref),
        (tab_hbm.at[me], tab), (inv_hbm, inv_ref),
    )
    small = [pltpu.make_async_copy(src, dst, small_sems.at[i]) for i, (src, dst) in enumerate(pairs)]
    for copy in small:
        copy.start()

    barrier = pltpu.get_barrier_semaphore()

    def away(k):
        return (
            ((me // 32 + k // 32) % 2 * 4 + (me // 8 + k // 8 % 4) % 4) * 4 + (me // 2 + k // 2 % 4) % 4
        ) * 2 + (me + k % 2) % 2

    def peer(i):
        return away((i * (i + 1) // 2) % PEERS)

    def greet(i, _):
        pl.semaphore_signal(barrier, inc=1, device_id={"rows": (me + i) % PEERS}, device_id_type=MESH)
        return 0

    lax.fori_loop(1, PEERS, greet, 0)

    small[0].wait()
    small[1].wait()
    my_taps[0:1, :] = row_taps[0:128].reshape(1, LANES)
    my_taps[1:2, :] = row_taps[128:256].reshape(1, LANES)
    padded = jnp.concatenate([col_taps[...].reshape(1, 32), jnp.zeros((1, 96), F32)], axis=1)
    my_taps[2:3, :] = pltpu.roll(padded, (me % 4) * 32, 1)
    my_taps[3:4, :] = jnp.zeros((1, LANES), F32)
    my_tap_rows = pl.ds(pl.multiple_of(chip * 4, 4), 4)
    taps[core, my_tap_rows, :] = my_taps[...]

    small[3].wait()
    pltpu.make_async_copy(xs.at[pl.ds(1, 32)], xs.at[pl.ds(1, 32)], in_sem).wait()

    def to_planes(i, _):
        pair = jnp.concatenate([xs[2 * i + 1], xs[2 * i + 2]], axis=1)
        out = jnp.dot(fwd_ref[...], jnp.concatenate(halves(pair), axis=0), preferred_element_type=F32)
        out = out[:LANES] + out[LANES:]
        for f in range(2):
            for r in range(2):
                planes[f, 2 * i + r] = out[f * PEERS : (f + 1) * PEERS, r * LANES : (r + 1) * LANES]
        return 0

    lax.fori_loop(0, 16, to_planes, 0, unroll=2)
    pl.semaphore_wait(barrier, PEERS - 1)

    def remote(src, dst, send, recv, to):
        return pltpu.make_async_remote_copy(
            src_ref=src, dst_ref=dst, send_sem=send, recv_sem=recv, device_id={"rows": to}, device_id_type=MESH
        )

    def send_taps(i, _):
        to = away((i * (i + 1) // 2) % 32 * 2)
        remote(my_taps, taps.at[core, my_tap_rows, :], tap_send, tap_recv, to).start()
        return 0

    lax.fori_loop(1, 32, send_taps, 0)

    for f in range(2):

        def send_plane(i, _):
            to = peer(i)
            remote(
                planes.at[f, :, to, :],
                got.at[f, pl.ds(pl.multiple_of(me * 32, 32), 32)],
                a_send.at[f],
                a_recv.at[f],
                to,
            ).start()
            return 0

        lax.fori_loop(1, PEERS, send_plane, 0)

    down = remote(xs.at[32], xs.at[0], halo_send.at[0], halo_recv.at[0], (me + 1) % PEERS)
    up = remote(xs.at[1], xs.at[33], halo_send.at[1], halo_recv.at[1], (me + PEERS - 1) % PEERS)
    down.start()
    up.start()

    for f in range(2):

        def own(r, _):
            got[f, pl.ds(me * 32 + r, 1), :] = planes[f, r, pl.ds(me, 1), :]
            return 0

        lax.fori_loop(0, 32, own, 0)

    small[4].wait()
    pltpu.make_async_copy(taps.at[0, pl.ds(0, 124)], taps.at[0, pl.ds(0, 124)], tap_recv).wait()
    share = remote(taps.at[core], taps.at[core], share_send, share_recv, sibling)
    share.start()
    share.wait()
    g = jnp.dot(tab[:, 0:LANES], taps[0], preferred_element_type=F32, precision=lax.Precision.HIGHEST)
    g = g + jnp.dot(tab[:, LANES:], taps[1], preferred_element_type=F32, precision=lax.Precision.HIGHEST)
    sign = (2 * core - 1).astype(F32)
    for f in range(2):
        gr, gi = g[2 * f : 2 * f + 1], g[2 * f + 1 : 2 * f + 2]
        wr, wi = tab[4 + 2 * f : 5 + 2 * f, 0:LANES], tab[5 + 2 * f : 6 + 2 * f, 0:LANES]
        same = toeplitz(jnp.concatenate([gr, wr * gr - wi * gi], axis=1))
        cross = toeplitz(jnp.concatenate([gi, wr * gi + wi * gr], axis=1) * sign)
        for r, value in enumerate((same, cross)):
            h, l = halves(value)
            right[f, r * LANES : (r + 1) * LANES, 0:LANES] = h
            right[f, r * LANES : (r + 1) * LANES, LANES : 2 * LANES] = l

    lines[...] = sum(taps[c, pl.ds(4 * e + 2, BLOCKS, stride=8), :] for e in range(2) for c in range(2))

    def block(d, _):
        line = jnp.concatenate([lines[pl.ds(d, 1), :], lines[pl.ds((d + BLOCKS - 1) % BLOCKS, 1), :]], axis=1)
        blocks[d] = toeplitz(line).T
        return 0

    lax.fori_loop(0, BLOCKS, block, 0)

    def block_spectrum(t, _):
        rows = pl.ds(pl.multiple_of(t * 16, 16), 16)
        freqs = rfft([blocks[d, rows, :] for d in range(BLOCKS)])
        zero = jnp.zeros((16, LANES), F32)
        for f in range(8):
            if f == 0:
                quads = ((freqs[0][0], zero), (zero, freqs[8][0]))
            else:
                quads = ((freqs[f][0], -freqs[f][1]), (freqs[f][1], freqs[f][0]))
            for r in range(2):
                for c in range(2):
                    h, l = halves(quads[r][c] * (1.0 / BLOCKS))
                    cols = slice(c * LANES, (c + 1) * LANES)
                    left[f, pl.ds(pl.multiple_of(r * LANES + t * 16, 16), 16), cols] = h
                    left[f, pl.ds(pl.multiple_of(256 + r * LANES + t * 16, 16), 16), cols] = l
        return 0

    lax.fori_loop(0, 8, block_spectrum, 0)

    for f in range(2):
        pltpu.make_async_copy(got.at[f, pl.ds(0, 2016)], got.at[f, pl.ds(0, 2016)], a_recv.at[f]).wait()

        def spectrum(t, _):
            freqs = rfft(
                [got[f, pl.ds(pl.multiple_of(b * LANES + t * 16, 16), 16), :] for b in range(BLOCKS)]
            )
            for k in range(8):
                pair = (freqs[0][0], freqs[8][0]) if k == 0 else freqs[k]
                for r in range(2):
                    h, l = halves(pair[r])
                    rows = pl.ds(pl.multiple_of(r * LANES + t * 16, 16), 16)
                    spec[k, rows, 0:LANES] = h
                    spec[k, rows, LANES : 2 * LANES] = l
            return 0

        lax.fori_loop(0, 8, spectrum, 0)

        def multiply(k, _):
            out = jnp.dot(left[k], spec[k], preferred_element_type=F32)
            out = out[:256] + out[256:]
            prod[k] = out[:, :LANES] + out[:, LANES:]
            return 0

        lax.fori_loop(0, 8, multiply, 0)

        def unspectrum(t, _):
            freqs = []
            for k in range(9):
                re = prod[k % 8, pl.ds(pl.multiple_of((k // 8) * LANES + t * 16, 16), 16), :]
                im = None
                if k % 8:
                    im = prod[k, pl.ds(pl.multiple_of(LANES + t * 16, 16), 16), :]
                freqs.append((re, im))
            for b, value in enumerate(irfft(freqs)):
                done[f, pl.ds(pl.multiple_of(b * LANES + t * 16, 16), 16), :] = value
            return 0

        lax.fori_loop(0, 8, unspectrum, 0)
        swap = remote(done.at[f], other.at[f], swap_send.at[f], swap_recv.at[f], sibling)
        swap.start()
        swap.wait()

        def product(owners):
            rows = [pl.ds(pl.multiple_of(t * 32, 32), 32) for t in owners]
            both = [
                jnp.concatenate([ref[f, r, :] for r in rows], axis=0) for ref in (done, other)
            ]
            h, l = halves(jnp.concatenate(both, axis=1))
            out = jnp.dot(h, right[f], preferred_element_type=F32)
            return out[:, :LANES] + out[:, LANES:] + jnp.dot(l, right[f, :, 0:LANES], preferred_element_type=F32)

        def send_back(j, _):
            owners = [peer(j * GROUP + 1 + k) for k in range(GROUP)]
            out = product(owners)
            for k, to in enumerate(owners):
                rows = pl.ds(pl.multiple_of(to * 32, 32), 32)
                sent[f, rows, :] = out[k * 32 : (k + 1) * 32]
                remote(sent.at[f, rows], back.at[f, :, me, :], b_send.at[f], b_recv.at[f], to).start()
            return 0

        lax.fori_loop(0, (PEERS - 1) // GROUP, send_back, 0)
        mine = product([me])
        for r in range(32):
            back[f, r, pl.ds(me, 1), :] = mine[r : r + 1]

    small[2].wait()
    small[5].wait()
    down.wait()
    up.wait()
    lane = lax.broadcasted_iota(jnp.int32, (LANES, LANES), 1)

    def stencil_row(y, _):
        total = jnp.zeros((LANES, LANES), F32)
        for a in range(3):
            here = xs[y + a]
            before, after = pltpu.roll(here, 1, 1), pltpu.roll(here, LANES - 1, 1)
            before = jnp.where(lane == 0, pltpu.roll(before, 1, 0), before)
            after = jnp.where(lane == LANES - 1, pltpu.roll(after, LANES - 1, 0), after)
            total = total + stencil[a, 0] * before + stencil[a, 1] * here + stencil[a, 2] * after
        local[y] = total
        return 0

    lax.fori_loop(0, 32, stencil_row, 0)

    for f in range(2):
        pltpu.make_async_copy(got.at[f, pl.ds(0, 2016)], got.at[f, pl.ds(0, 2016)], a_send.at[f]).wait()
    pltpu.make_async_copy(taps.at[0, pl.ds(0, 124)], taps.at[0, pl.ds(0, 124)], tap_send).wait()

    for f in range(2):
        pltpu.make_async_copy(got.at[f, pl.ds(0, 2016)], got.at[f, pl.ds(0, 2016)], b_recv.at[f]).wait()

        def from_planes(i, _):
            pair = jnp.concatenate([back[f, 2 * i], back[f, 2 * i + 1]], axis=1)
            h, l = halves(pair)
            out = jnp.dot(inv_ref[f], jnp.concatenate([h, l, h], axis=0), preferred_element_type=F32)
            local[2 * i] += out[:, :LANES]
            local[2 * i + 1] += out[:, LANES:]
            return 0

        lax.fori_loop(0, 16, from_planes, 0, unroll=2)

    def store(p, _):
        pltpu.make_async_copy(
            local.at[:, p, :], out_hbm.at[:, pl.ds(pl.multiple_of(p * LANES, LANES), LANES)], out_sem
        ).start()
        return 0

    lax.fori_loop(0, LANES, store, 0, unroll=8)
    for f in range(2):
        pltpu.make_async_copy(got.at[f, pl.ds(0, 2016)], got.at[f, pl.ds(0, 2016)], b_send.at[f]).wait()
    pltpu.make_async_copy(local, local, out_sem).wait()


def body(pixels, row_taps, column_taps, stencil):
    fwd, inv = plane_tables()
    hbm = pl.BlockSpec(memory_space=pltpu.HBM)
    block = (32, LANES, LANES)
    columns = (2, 2048, LANES)
    dma = pltpu.SemaphoreType.DMA
    return pl.pallas_call(
        kernel,
        out_shape=jax.ShapeDtypeStruct(pixels.shape, F32),
        in_specs=[hbm] * 7,
        out_specs=hbm,
        scratch_shapes=[
            pltpu.VMEM((256,), F32),
            pltpu.VMEM((32,), F32),
            pltpu.SMEM((3, 3), F32),
            pltpu.VMEM((256, 256), BF16),
            pltpu.VMEM((2, LANES, 192), BF16),
            pltpu.VMEM((8, 2 * LANES), F32),
            pltpu.VMEM((4, LANES), F32),
            pltpu.VMEM((2, LANES, LANES), F32),
            pltpu.VMEM((34, LANES, LANES), F32),
            pltpu.VMEM((2, 32, PEERS, LANES), F32),
            pltpu.VMEM(columns, F32),
            pltpu.VMEM(columns, F32),
            pltpu.VMEM(columns, F32),
            pltpu.VMEM(columns, F32),
            pltpu.VMEM((2, 32, PEERS, LANES), F32),
            pltpu.VMEM(block, F32),
            pltpu.VMEM((BLOCKS, LANES), F32),
            pltpu.VMEM((BLOCKS, LANES, LANES), F32),
            pltpu.VMEM((8, 512, 256), BF16),
            pltpu.VMEM((8, 256, 256), BF16),
            pltpu.VMEM((8, 256, LANES), F32),
            pltpu.VMEM((2, 256, 256), BF16),
            dma, dma, dma((6,)), dma, dma, dma, dma, dma((2,)), dma((2,)),
            dma((2,)), dma((2,)), dma((2,)), dma((2,)), dma((2,)), dma((2,)),
        ],
        compiler_params=pltpu.CompilerParams(
            collective_id=0, has_side_effects=True, vmem_limit_bytes=67_043_328
        ),
        name="filter_rows_and_columns",
    )(pixels, row_taps, column_taps, stencil, jnp.asarray(tap_tables()), jnp.asarray(fwd), jnp.asarray(inv))


def solution(mesh):
    in_specs = (
        P(("chan", "rows"), None),
        P(("chan", "rows")),
        P(("chan", "rows")),
        P("chan", None),
    )
    return jax.shard_map(
        body, mesh=mesh, in_specs=in_specs, out_specs=P(("chan", "rows"), None), check_vma=False
    )
```

```python
import math

import jax
import jax.numpy as jnp
import ml_dtypes
import numpy as np
from jax import lax
from jax.experimental import pallas as pl
from jax.experimental.pallas import tpu as pltpu
from jax.sharding import PartitionSpec as P

MESH = pl.DeviceIdType.MESH
F32, BF16 = jnp.float32, jnp.bfloat16
PEERS = 64
LANES = 128
BLOCKS = 16
MAIN_LIMIT = 67_043_328
FINISH_LIMIT = 67_043_328
PARTS = 1
GROUP = 7


STEPS = [(i * (i + 1) // 2) % PEERS for i in range(1, PEERS)]


def split_np(values):
    high = values.astype(ml_dtypes.bfloat16)
    low = (values - high.astype(np.float64)).astype(ml_dtypes.bfloat16)
    return high, low


def frequency(device, phase):
    return LANES // 2 if device == 1 and phase == 0 else 2 * (device // 2) + phase


def plane_tables():
    pos = np.arange(LANES)
    fwd = np.zeros((2, PEERS, LANES))
    inv = np.zeros((2, LANES, PEERS))
    for phase in range(2):
        for device in range(PEERS):
            freq = frequency(device, phase)
            angle = 2 * np.pi * (pos * freq % LANES) / LANES
            real = freq in (0, LANES // 2)
            wave = -np.sin(angle) if device % 2 and not real else np.cos(angle)
            fwd[phase, device] = wave
            inv[phase, :, device] = wave * (1 if real else 2) / LANES
    high, low = split_np(fwd.reshape(LANES, LANES))
    forward = np.block([[high, high], [low, low]])
    high, low = split_np(inv)
    return forward, np.concatenate([high, high, low], axis=2)


def tap_tables():
    tab = np.zeros((PEERS, 8, 2 * LANES), np.float64)
    pos = np.arange(LANES)
    cols = pos // 2 % 2 * LANES + pos // 4 * 4 + pos % 2
    for device in range(PEERS):
        for phase in range(2):
            freq = frequency(device, phase)
            angle = 2 * np.pi * (pos * freq % LANES) / LANES
            tab[device, 2 * phase, cols], tab[device, 2 * phase + 1, cols] = np.cos(angle), -np.sin(angle)
            turn = 2 * np.pi * freq / LANES
            tab[device, 4 + 2 * phase], tab[device, 5 + 2 * phase] = np.cos(turn), -np.sin(turn)
    return tab.astype(np.float32)


def turned(k, n, re, im, sign):
    angle = 2 * math.pi * k / n
    c, s = math.cos(angle), sign * math.sin(angle)
    if k == 0:
        return re, im
    if 4 * k == n:
        return (-im, re) if sign > 0 else (im, -re)
    if 8 * k == n:
        return (re - s / abs(s) * im) * c, (im + s / abs(s) * re) * c
    return re * c - im * s, re * s + im * c


def rfft(values):
    n = len(values)
    if n == 2:
        return [(values[0] + values[1], None), (values[0] - values[1], None)]
    even, odd = rfft(values[0::2]), rfft(values[1::2])
    out = [None] * (n // 2 + 1)
    for k in range(n // 4 + 1):
        er, ei = even[k]
        orr, oi = odd[k]
        if k == 0:
            out[0], out[n // 2] = (er + orr, None), (er - orr, None)
        elif 4 * k == n:
            out[k] = (er, -orr)
        else:
            tr, ti = turned(k, n, orr, oi, -1)
            out[k] = (er + tr, ei + ti)
            out[n // 2 - k] = (er - tr, ti - ei)
    return out


def irfft(spectrum):
    n = 2 * (len(spectrum) - 1)
    if n == 2:
        a, b = spectrum[0][0], spectrum[1][0]
        return [a + b, a - b]
    even, odd = [None] * (n // 4 + 1), [None] * (n // 4 + 1)
    for k in range(n // 4 + 1):
        ar, ai = spectrum[k]
        br, bi = spectrum[n // 2 - k]
        if k == 0:
            even[0], odd[0] = (ar + br, None), (ar - br, None)
        elif 4 * k == n:
            even[k], odd[k] = (2.0 * ar, None), (-2.0 * ai, None)
        else:
            even[k] = (ar + br, ai - bi)
            odd[k] = turned(k, n, ar - br, ai + bi, +1)
    out = [None] * n
    out[0::2], out[1::2] = irfft(even), irfft(odd)
    return out


def halves(value):
    high = value.astype(BF16)
    return high, (value - high.astype(F32)).astype(BF16)


def toeplitz(line):
    wide = jnp.broadcast_to(line, (LANES, 2 * LANES))
    return pltpu.roll(wide, 0, 1, stride=1, stride_axis=0)[:, :LANES]


def add_planes(table_ref, planes, base, total):
    def step(i, _):
        h, l = halves(jnp.concatenate([planes[2 * i], planes[2 * i + 1]], axis=1))
        out = jnp.dot(table_ref[...], jnp.concatenate([h, l, h], axis=0), preferred_element_type=F32)
        total[2 * i] = base[2 * i] + out[:, :LANES]
        total[2 * i + 1] = base[2 * i + 1] + out[:, LANES:]
        return 0

    lax.fori_loop(0, total.shape[0] // 2, step, 0, unroll=4)


def kernel(
    x_hbm, row_taps_hbm, col_taps_hbm, stencil_hbm, tab_hbm, fwd_hbm, inv_hbm, local_hbm, last,
    row_taps, col_taps, stencil, fwd_ref, inv_ref, tab, my_taps, taps,
    xs, planes, got, done, other, sent, first, local, lines, blocks, left, spec, prod, right,
    in_sem, out_sems, small_sems, tap_send, tap_recv, share_send, share_recv, halo_send, halo_recv,
    a_send, a_recv, swap_send, swap_recv, b_send, b_recv,
):
    me = lax.axis_index("rows")
    core, chip = me % 2, me // 2
    back = (first, last)
    sibling = chip * 2 + 1 - core

    def load(p, _):
        pltpu.make_async_copy(
            x_hbm.at[:, pl.ds(pl.multiple_of(p * LANES, LANES), LANES)], xs.at[pl.ds(1, 32), p, :], in_sem
        ).start()
        return 0

    lax.fori_loop(0, LANES, load, 0, unroll=8)
    pairs = (
        (row_taps_hbm, row_taps), (col_taps_hbm, col_taps), (stencil_hbm, stencil), (fwd_hbm, fwd_ref),
        (tab_hbm.at[me], tab), (inv_hbm, inv_ref),
    )
    small = [pltpu.make_async_copy(src, dst, small_sems.at[i]) for i, (src, dst) in enumerate(pairs)]
    for copy in small:
        copy.start()

    barrier = pltpu.get_barrier_semaphore()

    ys = [(me // 32 + k) % 2 * 32 for k in range(2)]
    xs_at = [(me // 8 + k) % 4 * 8 for k in range(4)]
    zs = [(me // 2 + k) % 4 * 2 for k in range(4)]
    cores = [(me + k) % 2 for k in range(2)]
    peers = [ys[k // 32] + xs_at[k // 8 % 4] + zs[k // 2 % 4] + cores[k % 2] for k in STEPS]

    for to in peers:
        pl.semaphore_signal(barrier, inc=1, device_id={"rows": to}, device_id_type=MESH)

    small[0].wait()
    small[1].wait()
    my_taps[0:1, :] = row_taps[0:128].reshape(1, LANES)
    my_taps[1:2, :] = row_taps[128:256].reshape(1, LANES)
    padded = jnp.concatenate([col_taps[...].reshape(1, 32), jnp.zeros((1, 96), F32)], axis=1)
    my_taps[2:3, :] = pltpu.roll(padded, (me % 4) * 32, 1)
    my_taps[3:4, :] = jnp.zeros((1, LANES), F32)
    my_tap_rows = pl.ds(pl.multiple_of(chip * 4, 4), 4)
    taps[core, my_tap_rows, :] = my_taps[...]

    small[3].wait()
    pltpu.make_async_copy(xs.at[pl.ds(1, 32)], xs.at[pl.ds(1, 32)], in_sem).wait()

    def to_planes(i, _):
        pair = jnp.concatenate([xs[2 * i + 1], xs[2 * i + 2]], axis=1)
        out = jnp.dot(fwd_ref[...], jnp.concatenate(halves(pair), axis=0), preferred_element_type=F32)
        out = out[:LANES] + out[LANES:]
        for f in range(2):
            for r in range(2):
                planes[f, 2 * i + r] = out[f * PEERS : (f + 1) * PEERS, r * LANES : (r + 1) * LANES]
        return 0

    lax.fori_loop(0, 16, to_planes, 0, unroll=4)
    pl.semaphore_wait(barrier, PEERS - 1)

    def remote(src, dst, send, recv, to):
        return pltpu.make_async_remote_copy(
            src_ref=src, dst_ref=dst, send_sem=send, recv_sem=recv, device_id={"rows": to}, device_id_type=MESH
        )

    for step, to in zip(STEPS, peers):
        if step % 2 == 0:
            remote(my_taps, taps.at[core, my_tap_rows, :], tap_send, tap_recv, to).start()
    for f in range(2):
        for to in peers:
            remote(
                planes.at[f, :, to, :],
                got.at[f, pl.ds(pl.multiple_of(me * 32, 32), 32)],
                a_send.at[f],
                a_recv.at[f],
                to,
            ).start()

    down = remote(xs.at[32], xs.at[0], halo_send.at[0], halo_recv.at[0], (me + 1) % PEERS)
    up = remote(xs.at[1], xs.at[33], halo_send.at[1], halo_recv.at[1], (me + PEERS - 1) % PEERS)
    down.start()
    up.start()

    for f in range(2):

        def own(r, _):
            got[f, pl.ds(me * 32 + r, 1), :] = planes[f, r, pl.ds(me, 1), :]
            return 0

        lax.fori_loop(0, 32, own, 0)

    small[4].wait()
    pltpu.make_async_copy(taps.at[0, pl.ds(0, 124)], taps.at[0, pl.ds(0, 124)], tap_recv).wait()
    share = remote(taps.at[core], taps.at[core], share_send, share_recv, sibling)
    share.start()
    share.wait()
    g = jnp.dot(tab[:, 0:LANES], taps[0], preferred_element_type=F32, precision=lax.Precision.HIGHEST)
    g = g + jnp.dot(tab[:, LANES:], taps[1], preferred_element_type=F32, precision=lax.Precision.HIGHEST)
    sign = (2 * core - 1).astype(F32)
    for f in range(2):
        gr, gi = g[2 * f : 2 * f + 1], g[2 * f + 1 : 2 * f + 2]
        wr, wi = tab[4 + 2 * f : 5 + 2 * f, 0:LANES], tab[5 + 2 * f : 6 + 2 * f, 0:LANES]
        same = toeplitz(jnp.concatenate([gr, wr * gr - wi * gi], axis=1))
        cross = toeplitz(jnp.concatenate([gi, wr * gi + wi * gr], axis=1) * sign)
        for r, value in enumerate((same, cross)):
            h, l = halves(value)
            right[f, r * LANES : (r + 1) * LANES, 0:LANES] = h
            right[f, r * LANES : (r + 1) * LANES, LANES : 2 * LANES] = l

    lines[...] = sum(taps[c, pl.ds(4 * e + 2, BLOCKS, stride=8), :] for e in range(2) for c in range(2))

    def block(d, _):
        line = jnp.concatenate([lines[pl.ds(d, 1), :], lines[pl.ds((d + BLOCKS - 1) % BLOCKS, 1), :]], axis=1)
        blocks[d] = toeplitz(line).T
        return 0

    lax.fori_loop(0, BLOCKS, block, 0)

    def block_spectrum(t, _):
        rows = pl.ds(pl.multiple_of(t * 16, 16), 16)
        freqs = rfft([blocks[d, rows, :] for d in range(BLOCKS)])
        zero = jnp.zeros((16, LANES), F32)
        for f in range(8):
            if f == 0:
                quads = ((freqs[0][0], zero), (zero, freqs[8][0]))
            else:
                quads = ((freqs[f][0], -freqs[f][1]), (freqs[f][1], freqs[f][0]))
            for r in range(2):
                for c in range(2):
                    h, l = halves(quads[r][c] * (1.0 / BLOCKS))
                    cols = slice(c * LANES, (c + 1) * LANES)
                    left[f, pl.ds(pl.multiple_of(r * LANES + t * 16, 16), 16), cols] = h
                    left[f, pl.ds(pl.multiple_of(256 + r * LANES + t * 16, 16), 16), cols] = l
        return 0

    lax.fori_loop(0, 8, block_spectrum, 0)

    for f in range(2):
        pltpu.make_async_copy(got.at[f, pl.ds(0, 2016)], got.at[f, pl.ds(0, 2016)], a_recv.at[f]).wait()

        def spectrum(t, _):
            freqs = rfft(
                [got[f, pl.ds(pl.multiple_of(b * LANES + t * 16, 16), 16), :] for b in range(BLOCKS)]
            )
            for k in range(8):
                pair = (freqs[0][0], freqs[8][0]) if k == 0 else freqs[k]
                for r in range(2):
                    h, l = halves(pair[r])
                    rows = pl.ds(pl.multiple_of(r * LANES + t * 16, 16), 16)
                    spec[k, rows, 0:LANES] = h
                    spec[k, rows, LANES : 2 * LANES] = l
            return 0

        lax.fori_loop(0, 8, spectrum, 0)

        def multiply(k, _):
            out = jnp.dot(left[k], spec[k], preferred_element_type=F32)
            out = out[:256] + out[256:]
            prod[k] = out[:, :LANES] + out[:, LANES:]
            return 0

        lax.fori_loop(0, 8, multiply, 0)

        def unspectrum(t, _):
            freqs = []
            for k in range(9):
                re = prod[k % 8, pl.ds(pl.multiple_of((k // 8) * LANES + t * 16, 16), 16), :]
                im = None
                if k % 8:
                    im = prod[k, pl.ds(pl.multiple_of(LANES + t * 16, 16), 16), :]
                freqs.append((re, im))
            for b, value in enumerate(irfft(freqs)):
                done[f, pl.ds(pl.multiple_of(b * LANES + t * 16, 16), 16), :] = value
            return 0

        lax.fori_loop(0, 8, unspectrum, 0)
        swap = remote(done.at[f], other.at[f], swap_send.at[f], swap_recv.at[f], sibling)
        swap.start()
        swap.wait()

        def product(owners):
            rows = [pl.ds(pl.multiple_of(t * 32, 32), 32) for t in owners]
            both = [
                jnp.concatenate([ref[f, r, :] for r in rows], axis=0) for ref in (done, other)
            ]
            h, l = halves(jnp.concatenate(both, axis=1))
            out = jnp.dot(h, right[f], preferred_element_type=F32)
            return out[:, :LANES] + out[:, LANES:] + jnp.dot(l, right[f, :, 0:LANES], preferred_element_type=F32)

        for j in range(0, PEERS - 1, GROUP):
            owners = peers[j : j + GROUP]
            out = product(owners)
            for k, to in enumerate(owners):
                rows = pl.ds(pl.multiple_of(to * 32, 32), 32)
                sent[f, rows, :] = out[k * 32 : (k + 1) * 32]
                remote(sent.at[f, rows], back[f].at[:, me, :], b_send.at[f], b_recv.at[f], to).start()

        mine = product([me])
        if f == 0:
            for r in range(32):
                first[r, pl.ds(me, 1), :] = mine[r : r + 1]
        else:
            rows = pl.ds(pl.multiple_of(me * 32, 32), 32)
            sent[f, rows, :] = mine
            keep = pltpu.make_async_copy(sent.at[f, rows], last.at[:, me, :], out_sems.at[0])
            keep.start()

    small[2].wait()
    small[5].wait()
    down.wait()
    up.wait()
    lane = lax.broadcasted_iota(jnp.int32, (LANES, LANES), 1)

    def stencil_row(y, _):
        total = jnp.zeros((LANES, LANES), F32)
        for a in range(3):
            here = xs[y + a]
            before, after = pltpu.roll(here, 1, 1), pltpu.roll(here, LANES - 1, 1)
            before = jnp.where(lane == 0, pltpu.roll(before, 1, 0), before)
            after = jnp.where(lane == LANES - 1, pltpu.roll(after, LANES - 1, 0), after)
            total = total + stencil[a, 0] * before + stencil[a, 1] * here + stencil[a, 2] * after
        local[y] = total
        return 0

    lax.fori_loop(0, 32, stencil_row, 0)

    for f in range(2):
        pltpu.make_async_copy(got.at[f, pl.ds(0, 2016)], got.at[f, pl.ds(0, 2016)], a_send.at[f]).wait()
    pltpu.make_async_copy(taps.at[0, pl.ds(0, 124)], taps.at[0, pl.ds(0, 124)], tap_send).wait()

    pltpu.make_async_copy(got.at[0, pl.ds(0, 2016)], got.at[0, pl.ds(0, 2016)], b_recv.at[0]).wait()
    add_planes(inv_ref, first, local, local)
    put = pltpu.make_async_copy(local, local_hbm, out_sems.at[1])
    put.start()
    for f in range(2):
        pltpu.make_async_copy(got.at[f, pl.ds(0, 2016)], got.at[f, pl.ds(0, 2016)], b_send.at[f]).wait()
    keep.wait()
    put.wait()
    pltpu.make_async_copy(got.at[1, pl.ds(0, 2016)], got.at[1, pl.ds(0, 2016)], b_recv.at[1]).wait()


def finish(local_hbm, last_hbm, inv_hbm, out_hbm, local, last, inv_ref, total, local_sems, last_sems, inv_sem, out_sem):
    table = pltpu.make_async_copy(inv_hbm, inv_ref, inv_sem)
    table.start()
    loads = []
    for i in range(PARTS):
        rows = pl.ds(i * 32 // PARTS, 32 // PARTS)
        loads.append(
            [
                pltpu.make_async_copy(last_hbm.at[rows], last.at[rows], last_sems.at[i]),
                pltpu.make_async_copy(local_hbm.at[rows], local.at[rows], local_sems.at[i]),
            ]
        )
        for copy in loads[i]:
            copy.start()
    table.wait()
    for i in range(PARTS):
        rows = pl.ds(i * 32 // PARTS, 32 // PARTS)
        for copy in loads[i]:
            copy.wait()
        add_planes(inv_ref, last.at[rows], local.at[rows], total.at[rows])

        def store(p, _):
            pltpu.make_async_copy(
                total.at[rows, p, :], out_hbm.at[rows, pl.ds(pl.multiple_of(p * LANES, LANES), LANES)], out_sem
            ).start()
            return 0

        lax.fori_loop(0, LANES, store, 0, unroll=16)
    pltpu.make_async_copy(total, total, out_sem).wait()


def body(pixels, row_taps, column_taps, stencil):
    fwd, inv = plane_tables()
    hbm = pl.BlockSpec(memory_space=pltpu.HBM)
    block = (32, LANES, LANES)
    half = (32, PEERS, LANES)
    columns = (2, 2048, LANES)
    dma = pltpu.SemaphoreType.DMA
    local, last = pl.pallas_call(
        kernel,
        out_shape=(jax.ShapeDtypeStruct(block, F32), jax.ShapeDtypeStruct(half, F32)),
        in_specs=[hbm] * 7,
        out_specs=(hbm, hbm),
        scratch_shapes=[
            pltpu.VMEM((256,), F32),
            pltpu.VMEM((32,), F32),
            pltpu.SMEM((3, 3), F32),
            pltpu.VMEM((256, 256), BF16),
            pltpu.VMEM((LANES, 192), BF16),
            pltpu.VMEM((8, 2 * LANES), F32),
            pltpu.VMEM((4, LANES), F32),
            pltpu.VMEM((2, LANES, LANES), F32),
            pltpu.VMEM((34, LANES, LANES), F32),
            pltpu.VMEM((2, 32, PEERS, LANES), F32),
            pltpu.VMEM(columns, F32),
            pltpu.VMEM(columns, F32),
            pltpu.VMEM(columns, F32),
            pltpu.VMEM(columns, F32),
            pltpu.VMEM(half, F32),
            pltpu.VMEM(block, F32),
            pltpu.VMEM((BLOCKS, LANES), F32),
            pltpu.VMEM((BLOCKS, LANES, LANES), F32),
            pltpu.VMEM((8, 512, 256), BF16),
            pltpu.VMEM((8, 256, 256), BF16),
            pltpu.VMEM((8, 256, LANES), F32),
            pltpu.VMEM((2, 256, 256), BF16),
            dma, dma((2,)), dma((6,)), dma, dma, dma, dma, dma((2,)), dma((2,)),
            dma((2,)), dma((2,)), dma((2,)), dma((2,)), dma((2,)), dma((2,)),
        ],
        compiler_params=pltpu.CompilerParams(
            collective_id=0, has_side_effects=True, vmem_limit_bytes=MAIN_LIMIT
        ),
        name="filter_rows_and_columns",
    )(pixels, row_taps, column_taps, stencil, jnp.asarray(tap_tables()), jnp.asarray(fwd), jnp.asarray(inv[0]))
    return pl.pallas_call(
        finish,
        out_shape=jax.ShapeDtypeStruct(pixels.shape, F32),
        in_specs=[hbm] * 3,
        out_specs=hbm,
        scratch_shapes=[
            pltpu.VMEM(block, F32),
            pltpu.VMEM(half, F32),
            pltpu.VMEM((LANES, 192), BF16),
            pltpu.VMEM(block, F32),
            dma((PARTS,)), dma((PARTS,)), dma, dma,
        ],
        compiler_params=pltpu.CompilerParams(vmem_limit_bytes=FINISH_LIMIT),
        name="last_planes",
    )(local, last, jnp.asarray(inv[1]))


def solution(mesh):
    in_specs = (
        P(("chan", "rows"), None),
        P(("chan", "rows")),
        P(("chan", "rows")),
        P("chan", None),
    )
    return jax.shard_map(
        body, mesh=mesh, in_specs=in_specs, out_specs=P(("chan", "rows"), None), check_vma=False
    )
```

```python
import math

import jax
import jax.numpy as jnp
import ml_dtypes
import numpy as np
from jax import lax
from jax.experimental import pallas as pl
from jax.experimental.pallas import tpu as pltpu
from jax.sharding import PartitionSpec as P

MESH = pl.DeviceIdType.MESH
F32, BF16 = jnp.float32, jnp.bfloat16
PEERS = 64
LANES = 128
BLOCKS = 16
MAIN_LIMIT = 48 * 2**20
FINISH_LIMIT = 32 * 2**20
PARTS = 1
GROUP = 7


STEPS = [(i * (i + 1) // 2) % PEERS for i in range(1, PEERS)]


def split_np(values):
    high = values.astype(ml_dtypes.bfloat16)
    low = (values - high.astype(np.float64)).astype(ml_dtypes.bfloat16)
    return high, low


def frequency(device, phase):
    return LANES // 2 if device == 1 and phase == 0 else 2 * (device // 2) + phase


def plane_tables():
    pos = np.arange(LANES)
    fwd = np.zeros((2, PEERS, LANES))
    inv = np.zeros((2, LANES, PEERS))
    for phase in range(2):
        for device in range(PEERS):
            freq = frequency(device, phase)
            angle = 2 * np.pi * (pos * freq % LANES) / LANES
            real = freq in (0, LANES // 2)
            wave = -np.sin(angle) if device % 2 and not real else np.cos(angle)
            fwd[phase, device] = wave
            inv[phase, :, device] = wave * (1 if real else 2) / LANES
    high, low = split_np(fwd.reshape(LANES, LANES))
    forward = np.block([[high, high], [low, low]])
    high, low = split_np(inv)
    return forward, np.concatenate([high, high, low], axis=2)


def tap_tables():
    tab = np.zeros((PEERS, 8, 2 * LANES), np.float64)
    pos = np.arange(LANES)
    cols = pos // 2 % 2 * LANES + pos // 4 * 4 + pos % 2
    for device in range(PEERS):
        for phase in range(2):
            freq = frequency(device, phase)
            angle = 2 * np.pi * (pos * freq % LANES) / LANES
            tab[device, 2 * phase, cols], tab[device, 2 * phase + 1, cols] = np.cos(angle), -np.sin(angle)
            turn = 2 * np.pi * freq / LANES
            tab[device, 4 + 2 * phase], tab[device, 5 + 2 * phase] = np.cos(turn), -np.sin(turn)
    return tab.astype(np.float32)


def turned(k, n, re, im, sign):
    angle = 2 * math.pi * k / n
    c, s = math.cos(angle), sign * math.sin(angle)
    if k == 0:
        return re, im
    if 4 * k == n:
        return (-im, re) if sign > 0 else (im, -re)
    if 8 * k == n:
        return (re - s / abs(s) * im) * c, (im + s / abs(s) * re) * c
    return re * c - im * s, re * s + im * c


def rfft(values):
    n = len(values)
    if n == 2:
        return [(values[0] + values[1], None), (values[0] - values[1], None)]
    even, odd = rfft(values[0::2]), rfft(values[1::2])
    out = [None] * (n // 2 + 1)
    for k in range(n // 4 + 1):
        er, ei = even[k]
        orr, oi = odd[k]
        if k == 0:
            out[0], out[n // 2] = (er + orr, None), (er - orr, None)
        elif 4 * k == n:
            out[k] = (er, -orr)
        else:
            tr, ti = turned(k, n, orr, oi, -1)
            out[k] = (er + tr, ei + ti)
            out[n // 2 - k] = (er - tr, ti - ei)
    return out


def irfft(spectrum):
    n = 2 * (len(spectrum) - 1)
    if n == 2:
        a, b = spectrum[0][0], spectrum[1][0]
        return [a + b, a - b]
    even, odd = [None] * (n // 4 + 1), [None] * (n // 4 + 1)
    for k in range(n // 4 + 1):
        ar, ai = spectrum[k]
        br, bi = spectrum[n // 2 - k]
        if k == 0:
            even[0], odd[0] = (ar + br, None), (ar - br, None)
        elif 4 * k == n:
            even[k], odd[k] = (2.0 * ar, None), (-2.0 * ai, None)
        else:
            even[k] = (ar + br, ai - bi)
            odd[k] = turned(k, n, ar - br, ai + bi, +1)
    out = [None] * n
    out[0::2], out[1::2] = irfft(even), irfft(odd)
    return out


def halves(value):
    high = value.astype(BF16)
    return high, (value - high.astype(F32)).astype(BF16)


def toeplitz(line):
    wide = jnp.broadcast_to(line, (LANES, 2 * LANES))
    return pltpu.roll(wide, 0, 1, stride=1, stride_axis=0)[:, :LANES]


def add_planes(table_ref, planes, base, total):
    def step(i, _):
        h, l = halves(jnp.concatenate([planes[2 * i], planes[2 * i + 1]], axis=1))
        out = jnp.dot(table_ref[...], jnp.concatenate([h, l, h], axis=0), preferred_element_type=F32)
        total[2 * i] = base[2 * i] + out[:, :LANES]
        total[2 * i + 1] = base[2 * i + 1] + out[:, LANES:]
        return 0

    lax.fori_loop(0, total.shape[0] // 2, step, 0, unroll=4)


def kernel(
    x_hbm, row_taps_hbm, col_taps_hbm, stencil_hbm, tab_hbm, fwd_hbm, inv_hbm, local, last,
    row_taps, col_taps, stencil, fwd_ref, inv_ref, tab, my_taps, taps,
    xs, planes, got, done, other, sent, first, lines, blocks, left, spec, prod, right,
    in_sems, small_sems, tap_send, tap_recv, share_send, share_recv, halo_send, halo_recv,
    a_send, a_recv, swap_send, swap_recv, b_send, b_recv,
):
    me = lax.axis_index("rows")
    core, chip = me % 2, me // 2
    back = (first, last)
    sibling = chip * 2 + 1 - core

    for y in range(32):
        pltpu.make_async_copy(x_hbm.at[y // 8, :, y % 8, :], xs.at[1 + y], in_sems.at[y // 8]).start()
    pairs = (
        (row_taps_hbm, row_taps), (col_taps_hbm, col_taps), (stencil_hbm, stencil), (fwd_hbm, fwd_ref),
        (tab_hbm.at[me], tab), (inv_hbm, inv_ref),
    )
    small = [pltpu.make_async_copy(src, dst, small_sems.at[i]) for i, (src, dst) in enumerate(pairs)]
    for copy in small:
        copy.start()

    barrier = pltpu.get_barrier_semaphore()

    ys = [(me // 32 + k) % 2 * 32 for k in range(2)]
    xs_at = [(me // 8 + k) % 4 * 8 for k in range(4)]
    zs = [(me // 2 + k) % 4 * 2 for k in range(4)]
    cores = [(me + k) % 2 for k in range(2)]
    peers = [ys[k // 32] + xs_at[k // 8 % 4] + zs[k // 2 % 4] + cores[k % 2] for k in STEPS]

    for to in peers:
        pl.semaphore_signal(barrier, inc=1, device_id={"rows": to}, device_id_type=MESH)

    small[0].wait()
    small[1].wait()
    my_taps[0:1, :] = row_taps[0:128].reshape(1, LANES)
    my_taps[1:2, :] = row_taps[128:256].reshape(1, LANES)
    padded = jnp.concatenate([col_taps[...].reshape(1, 32), jnp.zeros((1, 96), F32)], axis=1)
    my_taps[2:3, :] = pltpu.roll(padded, (me % 4) * 32, 1)
    my_taps[3:4, :] = jnp.zeros((1, LANES), F32)
    my_tap_rows = pl.ds(pl.multiple_of(chip * 4, 4), 4)
    taps[core, my_tap_rows, :] = my_taps[...]

    small[3].wait()

    def to_planes(i, _):
        pair = jnp.concatenate([xs[2 * i + 1], xs[2 * i + 2]], axis=1)
        out = jnp.dot(fwd_ref[...], jnp.concatenate(halves(pair), axis=0), preferred_element_type=F32)
        out = out[:LANES] + out[LANES:]
        for f in range(2):
            for r in range(2):
                planes[f, 2 * i + r] = out[f * PEERS : (f + 1) * PEERS, r * LANES : (r + 1) * LANES]
        return 0

    for part in range(4):
        rows = xs.at[pl.ds(1 + 8 * part, 8)]
        pltpu.make_async_copy(rows, rows, in_sems.at[part]).wait()
        lax.fori_loop(4 * part, 4 * part + 4, to_planes, 0, unroll=4)
    pl.semaphore_wait(barrier, PEERS - 1)

    def remote(src, dst, send, recv, to):
        return pltpu.make_async_remote_copy(
            src_ref=src, dst_ref=dst, send_sem=send, recv_sem=recv, device_id={"rows": to}, device_id_type=MESH
        )

    for step, to in zip(STEPS, peers):
        if step % 2 == 0:
            remote(my_taps, taps.at[core, my_tap_rows, :], tap_send, tap_recv, to).start()
    for f in range(2):
        for to in peers:
            remote(
                planes.at[f, :, to, :],
                got.at[f, pl.ds(pl.multiple_of(me * 32, 32), 32)],
                a_send.at[f],
                a_recv.at[f],
                to,
            ).start()

    down = remote(xs.at[32], xs.at[0], halo_send.at[0], halo_recv.at[0], (me + 1) % PEERS)
    up = remote(xs.at[1], xs.at[33], halo_send.at[1], halo_recv.at[1], (me + PEERS - 1) % PEERS)
    down.start()
    up.start()

    for f in range(2):

        def own(r, _):
            got[f, pl.ds(me * 32 + r, 1), :] = planes[f, r, pl.ds(me, 1), :]
            return 0

        lax.fori_loop(0, 32, own, 0)

    small[4].wait()
    pltpu.make_async_copy(taps.at[0, pl.ds(0, 124)], taps.at[0, pl.ds(0, 124)], tap_recv).wait()
    share = remote(taps.at[core], taps.at[core], share_send, share_recv, sibling)
    share.start()
    share.wait()
    g = jnp.dot(tab[:, 0:LANES], taps[0], preferred_element_type=F32, precision=lax.Precision.HIGHEST)
    g = g + jnp.dot(tab[:, LANES:], taps[1], preferred_element_type=F32, precision=lax.Precision.HIGHEST)
    sign = (2 * core - 1).astype(F32)
    for f in range(2):
        gr, gi = g[2 * f : 2 * f + 1], g[2 * f + 1 : 2 * f + 2]
        wr, wi = tab[4 + 2 * f : 5 + 2 * f, 0:LANES], tab[5 + 2 * f : 6 + 2 * f, 0:LANES]
        same = toeplitz(jnp.concatenate([gr, wr * gr - wi * gi], axis=1))
        cross = toeplitz(jnp.concatenate([gi, wr * gi + wi * gr], axis=1) * sign)
        for r, value in enumerate((same, cross)):
            h, l = halves(value)
            right[f, r * LANES : (r + 1) * LANES, 0:LANES] = h
            right[f, r * LANES : (r + 1) * LANES, LANES : 2 * LANES] = l

    lines[...] = sum(taps[c, pl.ds(4 * e + 2, BLOCKS, stride=8), :] for e in range(2) for c in range(2))

    def block(d, _):
        line = jnp.concatenate([lines[pl.ds(d, 1), :], lines[pl.ds((d + BLOCKS - 1) % BLOCKS, 1), :]], axis=1)
        blocks[d] = toeplitz(line).T
        return 0

    lax.fori_loop(0, BLOCKS, block, 0)

    def block_spectrum(t, _):
        rows = pl.ds(pl.multiple_of(t * 16, 16), 16)
        freqs = rfft([blocks[d, rows, :] for d in range(BLOCKS)])
        zero = jnp.zeros((16, LANES), F32)
        for f in range(8):
            if f == 0:
                quads = ((freqs[0][0], zero), (zero, freqs[8][0]))
            else:
                quads = ((freqs[f][0], -freqs[f][1]), (freqs[f][1], freqs[f][0]))
            for r in range(2):
                for c in range(2):
                    h, l = halves(quads[r][c] * (1.0 / BLOCKS))
                    cols = slice(c * LANES, (c + 1) * LANES)
                    left[f, pl.ds(pl.multiple_of(r * LANES + t * 16, 16), 16), cols] = h
                    left[f, pl.ds(pl.multiple_of(256 + r * LANES + t * 16, 16), 16), cols] = l
        return 0

    lax.fori_loop(0, 8, block_spectrum, 0)

    for f in range(2):
        pltpu.make_async_copy(got.at[f, pl.ds(0, 2016)], got.at[f, pl.ds(0, 2016)], a_recv.at[f]).wait()

        def spectrum(t, _):
            freqs = rfft(
                [got[f, pl.ds(pl.multiple_of(b * LANES + t * 16, 16), 16), :] for b in range(BLOCKS)]
            )
            for k in range(8):
                pair = (freqs[0][0], freqs[8][0]) if k == 0 else freqs[k]
                for r in range(2):
                    h, l = halves(pair[r])
                    rows = pl.ds(pl.multiple_of(r * LANES + t * 16, 16), 16)
                    spec[k, rows, 0:LANES] = h
                    spec[k, rows, LANES : 2 * LANES] = l
            return 0

        lax.fori_loop(0, 8, spectrum, 0)

        def multiply(k, _):
            out = jnp.dot(left[k], spec[k], preferred_element_type=F32)
            out = out[:256] + out[256:]
            prod[k] = out[:, :LANES] + out[:, LANES:]
            return 0

        lax.fori_loop(0, 8, multiply, 0)

        def unspectrum(t, _):
            freqs = []
            for k in range(9):
                re = prod[k % 8, pl.ds(pl.multiple_of((k // 8) * LANES + t * 16, 16), 16), :]
                im = None
                if k % 8:
                    im = prod[k, pl.ds(pl.multiple_of(LANES + t * 16, 16), 16), :]
                freqs.append((re, im))
            for b, value in enumerate(irfft(freqs)):
                done[f, pl.ds(pl.multiple_of(b * LANES + t * 16, 16), 16), :] = value
            return 0

        lax.fori_loop(0, 8, unspectrum, 0)
        swap = remote(done.at[f], other.at[f], swap_send.at[f], swap_recv.at[f], sibling)
        swap.start()
        swap.wait()

        def product(owners):
            rows = [pl.ds(pl.multiple_of(t * 32, 32), 32) for t in owners]
            both = [
                jnp.concatenate([ref[f, r, :] for r in rows], axis=0) for ref in (done, other)
            ]
            h, l = halves(jnp.concatenate(both, axis=1))
            out = jnp.dot(h, right[f], preferred_element_type=F32)
            return out[:, :LANES] + out[:, LANES:] + jnp.dot(l, right[f, :, 0:LANES], preferred_element_type=F32)

        def send_back(owners):
            for to in owners:
                rows = pl.ds(pl.multiple_of(to * 32, 32), 32)
                remote(sent.at[f, rows], back[f].at[:, me, :], b_send.at[f], b_recv.at[f], to).start()

        groups = [peers[j : j + GROUP] for j in range(0, PEERS - 1, GROUP)]
        for j, owners in enumerate(groups):
            out = product(owners)
            for k, to in enumerate(owners):
                sent[f, pl.ds(pl.multiple_of(to * 32, 32), 32), :] = out[k * 32 : (k + 1) * 32]
            if j:
                send_back(groups[j - 1])
        send_back(groups[-1])
        mine = product([me])
        for r in range(32):
            back[f][r, pl.ds(me, 1), :] = mine[r : r + 1]

    small[2].wait()
    small[5].wait()
    down.wait()
    up.wait()
    lane = lax.broadcasted_iota(jnp.int32, (LANES, LANES), 1)

    def stencil_row(y, _):
        total = jnp.zeros((LANES, LANES), F32)
        for a in range(3):
            here = xs[y + a]
            before, after = pltpu.roll(here, 1, 1), pltpu.roll(here, LANES - 1, 1)
            before = jnp.where(lane == 0, pltpu.roll(before, 1, 0), before)
            after = jnp.where(lane == LANES - 1, pltpu.roll(after, LANES - 1, 0), after)
            total = total + stencil[a, 0] * before + stencil[a, 1] * here + stencil[a, 2] * after
        local[y] = total
        return 0

    lax.fori_loop(0, 32, stencil_row, 0)

    for f in range(2):
        pltpu.make_async_copy(got.at[f, pl.ds(0, 2016)], got.at[f, pl.ds(0, 2016)], a_send.at[f]).wait()
    pltpu.make_async_copy(taps.at[0, pl.ds(0, 124)], taps.at[0, pl.ds(0, 124)], tap_send).wait()

    pltpu.make_async_copy(got.at[0, pl.ds(0, 2016)], got.at[0, pl.ds(0, 2016)], b_recv.at[0]).wait()
    add_planes(inv_ref, first, local, local)
    for f in range(2):
        pltpu.make_async_copy(got.at[f, pl.ds(0, 2016)], got.at[f, pl.ds(0, 2016)], b_send.at[f]).wait()
    pltpu.make_async_copy(got.at[1, pl.ds(0, 2016)], got.at[1, pl.ds(0, 2016)], b_recv.at[1]).wait()


def finish(local, last, inv_ref, out_hbm, total, out_sem):
    def store(y):
        pltpu.make_async_copy(total.at[y], out_hbm.at[y // 8, :, y % 8, :], out_sem).start()

    for part in range(PARTS):
        rows = pl.ds(part * 32 // PARTS, 32 // PARTS)
        add_planes(inv_ref, last.at[rows], local.at[rows], total.at[rows])
        for y in range(part * 32 // PARTS, (part + 1) * 32 // PARTS):
            store(y)
    pltpu.make_async_copy(total, total, out_sem).wait()


def tiles(image):
    return image.reshape(4, 8, LANES, LANES).transpose(0, 2, 1, 3)


def body(pixels, row_taps, column_taps, stencil):
    fwd, inv = plane_tables()
    hbm, vmem = pl.BlockSpec(memory_space=pltpu.HBM), pl.BlockSpec(memory_space=pltpu.VMEM)
    block = (32, LANES, LANES)
    half = (32, PEERS, LANES)
    columns = (2, 2048, LANES)
    dma = pltpu.SemaphoreType.DMA
    operands = (
        tiles(pixels), row_taps, column_taps, stencil,
        jnp.asarray(tap_tables()), jnp.asarray(fwd), jnp.asarray(inv[0]),
    )
    local, last = pl.pallas_call(
        kernel,
        out_shape=(pltpu.VMEM(block, F32), pltpu.VMEM(half, F32)),
        in_specs=[hbm] * 7,
        out_specs=(vmem, vmem),
        scratch_shapes=[
            pltpu.VMEM((256,), F32),
            pltpu.VMEM((32,), F32),
            pltpu.SMEM((3, 3), F32),
            pltpu.VMEM((256, 256), BF16),
            pltpu.VMEM((LANES, 192), BF16),
            pltpu.VMEM((8, 2 * LANES), F32),
            pltpu.VMEM((4, LANES), F32),
            pltpu.VMEM((2, LANES, LANES), F32),
            pltpu.VMEM((34, LANES, LANES), F32),
            pltpu.VMEM((2, 32, PEERS, LANES), F32),
            pltpu.VMEM(columns, F32),
            pltpu.VMEM(columns, F32),
            pltpu.VMEM(columns, F32),
            pltpu.VMEM(columns, F32),
            pltpu.VMEM(half, F32),
            pltpu.VMEM((BLOCKS, LANES), F32),
            pltpu.VMEM((BLOCKS, LANES, LANES), F32),
            pltpu.VMEM((8, 512, 256), BF16),
            pltpu.VMEM((8, 256, 256), BF16),
            pltpu.VMEM((8, 256, LANES), F32),
            pltpu.VMEM((2, 256, 256), BF16),
            dma((4,)), dma((6,)), dma, dma, dma, dma, dma((2,)), dma((2,)),
            dma((2,)), dma((2,)), dma((2,)), dma((2,)), dma((2,)), dma((2,)),
        ],
        compiler_params=pltpu.CompilerParams(
            collective_id=0, has_side_effects=True, vmem_limit_bytes=MAIN_LIMIT
        ),
        name="filter_rows_and_columns",
    )(*(pltpu.with_memory_space_constraint(operand, pltpu.HBM) for operand in operands))
    out = pl.pallas_call(
        finish,
        out_shape=jax.ShapeDtypeStruct((4, LANES, 8, LANES), F32),
        in_specs=[vmem] * 3,
        out_specs=hbm,
        scratch_shapes=[pltpu.VMEM(block, F32), dma],
        compiler_params=pltpu.CompilerParams(vmem_limit_bytes=FINISH_LIMIT),
        name="last_planes",
    )(local, last, jnp.asarray(inv[1]))
    return out.transpose(0, 2, 1, 3).reshape(pixels.shape)


def solution(mesh):
    in_specs = (
        P(("chan", "rows"), None),
        P(("chan", "rows")),
        P(("chan", "rows")),
        P("chan", None),
    )
    return jax.shard_map(
        body, mesh=mesh, in_specs=in_specs, out_specs=P(("chan", "rows"), None), check_vma=False
    )
```

```python
import math

import jax
import jax.numpy as jnp
import ml_dtypes
import numpy as np
from jax import lax
from jax.experimental import pallas as pl
from jax.experimental.pallas import tpu as pltpu
from jax.sharding import PartitionSpec as P

MESH = pl.DeviceIdType.MESH
F32, BF16 = jnp.float32, jnp.bfloat16
PEERS = 64
LANES = 128
BLOCKS = 16
MAIN_LIMIT = 48 * 2**20
FINISH_LIMIT = 32 * 2**20
PARTS = 4
GROUP = 7


STEPS = [
    52, 1, 53, 33, 21, 3, 55, 8, 61, 32, 20, 6, 50, 9, 60, 2,
    54, 25, 44, 7, 51, 24, 45, 35, 23, 30, 43, 27, 47, 5, 49, 11,
    63, 34, 22, 15, 58, 41, 28, 16, 36, 31, 42, 17, 37, 56, 12, 14,
    59, 26, 46, 38, 19, 57, 13, 39, 18, 10, 62, 40, 29, 4, 48,
]


def split_np(values):
    high = values.astype(ml_dtypes.bfloat16)
    low = (values - high.astype(np.float64)).astype(ml_dtypes.bfloat16)
    return high, low


def frequency(device, phase):
    return LANES // 2 if device == 1 and phase == 0 else 2 * (device // 2) + phase


def plane_tables():
    pos = np.arange(LANES)
    fwd = np.zeros((2, PEERS, LANES))
    inv = np.zeros((2, LANES, PEERS))
    for phase in range(2):
        for device in range(PEERS):
            freq = frequency(device, phase)
            angle = 2 * np.pi * (pos * freq % LANES) / LANES
            real = freq in (0, LANES // 2)
            wave = -np.sin(angle) if device % 2 and not real else np.cos(angle)
            fwd[phase, device] = wave
            inv[phase, :, device] = wave * (1 if real else 2) / LANES
    high, low = split_np(fwd.reshape(LANES, LANES))
    forward = np.block([[high, high], [low, low]])
    high, low = split_np(inv)
    return forward, np.concatenate([high, high, low], axis=2)


def tap_tables():
    tab = np.zeros((PEERS, 8, 2 * LANES), np.float64)
    pos = np.arange(LANES)
    cols = pos // 2 % 2 * LANES + pos // 4 * 4 + pos % 2
    for device in range(PEERS):
        for phase in range(2):
            freq = frequency(device, phase)
            angle = 2 * np.pi * (pos * freq % LANES) / LANES
            tab[device, 2 * phase, cols], tab[device, 2 * phase + 1, cols] = np.cos(angle), -np.sin(angle)
            turn = 2 * np.pi * freq / LANES
            tab[device, 4 + 2 * phase], tab[device, 5 + 2 * phase] = np.cos(turn), -np.sin(turn)
    return tab.astype(np.float32)


def turned(k, n, re, im, sign):
    angle = 2 * math.pi * k / n
    c, s = math.cos(angle), sign * math.sin(angle)
    if k == 0:
        return re, im
    if 4 * k == n:
        return (-im, re) if sign > 0 else (im, -re)
    if 8 * k == n:
        return (re - s / abs(s) * im) * c, (im + s / abs(s) * re) * c
    return re * c - im * s, re * s + im * c


def rfft(values):
    n = len(values)
    if n == 2:
        return [(values[0] + values[1], None), (values[0] - values[1], None)]
    even, odd = rfft(values[0::2]), rfft(values[1::2])
    out = [None] * (n // 2 + 1)
    for k in range(n // 4 + 1):
        er, ei = even[k]
        orr, oi = odd[k]
        if k == 0:
            out[0], out[n // 2] = (er + orr, None), (er - orr, None)
        elif 4 * k == n:
            out[k] = (er, -orr)
        else:
            tr, ti = turned(k, n, orr, oi, -1)
            out[k] = (er + tr, ei + ti)
            out[n // 2 - k] = (er - tr, ti - ei)
    return out


def irfft(spectrum):
    n = 2 * (len(spectrum) - 1)
    if n == 2:
        a, b = spectrum[0][0], spectrum[1][0]
        return [a + b, a - b]
    even, odd = [None] * (n // 4 + 1), [None] * (n // 4 + 1)
    for k in range(n // 4 + 1):
        ar, ai = spectrum[k]
        br, bi = spectrum[n // 2 - k]
        if k == 0:
            even[0], odd[0] = (ar + br, None), (ar - br, None)
        elif 4 * k == n:
            even[k], odd[k] = (2.0 * ar, None), (-2.0 * ai, None)
        else:
            even[k] = (ar + br, ai - bi)
            odd[k] = turned(k, n, ar - br, ai + bi, +1)
    out = [None] * n
    out[0::2], out[1::2] = irfft(even), irfft(odd)
    return out


def halves(value):
    high = value.astype(BF16)
    return high, (value - high.astype(F32)).astype(BF16)


def toeplitz(line):
    wide = jnp.broadcast_to(line, (LANES, 2 * LANES))
    return pltpu.roll(wide, 0, 1, stride=1, stride_axis=0)[:, :LANES]


def add_planes(table_ref, planes, base, total):
    def step(i, _):
        h, l = halves(jnp.concatenate([planes[2 * i], planes[2 * i + 1]], axis=1))
        out = jnp.dot(table_ref[...], jnp.concatenate([h, l, h], axis=0), preferred_element_type=F32)
        total[2 * i] = base[2 * i] + out[:, :LANES]
        total[2 * i + 1] = base[2 * i + 1] + out[:, LANES:]
        return 0

    lax.fori_loop(0, total.shape[0] // 2, step, 0, unroll=4)


def kernel(
    x_hbm, row_taps_hbm, col_taps_hbm, stencil_hbm, tab_hbm, fwd_hbm, inv_hbm, local, last,
    row_taps, col_taps, stencil, fwd_ref, inv_ref, tab, my_taps, taps,
    xs, planes, got, done, other, sent, first, lines, blocks, left, spec, prod, right,
    in_sem, small_sems, tap_send, tap_recv, share_send, share_recv, halo_send, halo_recv,
    a_send, a_recv, swap_send, swap_recv, b_send, b_recv,
):
    me = lax.axis_index("rows")
    core, chip = me % 2, me // 2
    back = (first, last)
    sibling = chip * 2 + 1 - core

    for y in range(32):
        pltpu.make_async_copy(x_hbm.at[y // 8, :, y % 8, :], xs.at[1 + y], in_sem).start()
    pairs = (
        (row_taps_hbm, row_taps), (col_taps_hbm, col_taps), (stencil_hbm, stencil), (fwd_hbm, fwd_ref),
        (tab_hbm.at[me], tab), (inv_hbm, inv_ref),
    )
    small = [pltpu.make_async_copy(src, dst, small_sems.at[i]) for i, (src, dst) in enumerate(pairs)]
    for copy in small:
        copy.start()

    barrier = pltpu.get_barrier_semaphore()

    ys = [(me // 32 + k) % 2 * 32 for k in range(2)]
    xs_at = [(me // 8 + k) % 4 * 8 for k in range(4)]
    zs = [(me // 2 + k) % 4 * 2 for k in range(4)]
    cores = [(me + k) % 2 for k in range(2)]
    peers = [ys[k // 32] + xs_at[k // 8 % 4] + zs[k // 2 % 4] + cores[k % 2] for k in STEPS]

    for to in peers:
        pl.semaphore_signal(barrier, inc=1, device_id={"rows": to}, device_id_type=MESH)

    small[0].wait()
    small[1].wait()
    my_taps[0:1, :] = row_taps[0:128].reshape(1, LANES)
    my_taps[1:2, :] = row_taps[128:256].reshape(1, LANES)
    padded = jnp.concatenate([col_taps[...].reshape(1, 32), jnp.zeros((1, 96), F32)], axis=1)
    my_taps[2:3, :] = pltpu.roll(padded, (me % 4) * 32, 1)
    my_taps[3:4, :] = jnp.zeros((1, LANES), F32)
    my_tap_rows = pl.ds(pl.multiple_of(chip * 4, 4), 4)
    taps[core, my_tap_rows, :] = my_taps[...]

    small[3].wait()

    def to_planes(i, _):
        pair = jnp.concatenate([xs[2 * i + 1], xs[2 * i + 2]], axis=1)
        out = jnp.dot(fwd_ref[...], jnp.concatenate(halves(pair), axis=0), preferred_element_type=F32)
        out = out[:LANES] + out[LANES:]
        for f in range(2):
            for r in range(2):
                planes[f, 2 * i + r] = out[f * PEERS : (f + 1) * PEERS, r * LANES : (r + 1) * LANES]
        return 0

    rows = xs.at[pl.ds(1, 32)]
    pltpu.make_async_copy(rows, rows, in_sem).wait()
    lax.fori_loop(0, 16, to_planes, 0, unroll=16)
    pl.semaphore_wait(barrier, PEERS - 1)

    def remote(src, dst, send, recv, to):
        return pltpu.make_async_remote_copy(
            src_ref=src, dst_ref=dst, send_sem=send, recv_sem=recv, device_id={"rows": to}, device_id_type=MESH
        )

    for step, to in zip(STEPS, peers):
        if step % 2 == 0:
            remote(my_taps, taps.at[core, my_tap_rows, :], tap_send, tap_recv, to).start()
    for f in range(2):
        for to in peers:
            remote(
                planes.at[f, :, to, :],
                got.at[f, pl.ds(pl.multiple_of(me * 32, 32), 32)],
                a_send.at[f],
                a_recv.at[f],
                to,
            ).start()

    down = remote(xs.at[32], xs.at[0], halo_send.at[0], halo_recv.at[0], (me + 1) % PEERS)
    up = remote(xs.at[1], xs.at[33], halo_send.at[1], halo_recv.at[1], (me + PEERS - 1) % PEERS)
    down.start()
    up.start()

    for f in range(2):

        def own(r, _):
            got[f, pl.ds(me * 32 + r, 1), :] = planes[f, r, pl.ds(me, 1), :]
            return 0

        lax.fori_loop(0, 32, own, 0)

    small[4].wait()
    pltpu.make_async_copy(taps.at[0, pl.ds(0, 124)], taps.at[0, pl.ds(0, 124)], tap_recv).wait()
    share = remote(taps.at[core], taps.at[core], share_send, share_recv, sibling)
    share.start()
    share.wait()
    g = jnp.dot(tab[:, 0:LANES], taps[0], preferred_element_type=F32, precision=lax.Precision.HIGHEST)
    g = g + jnp.dot(tab[:, LANES:], taps[1], preferred_element_type=F32, precision=lax.Precision.HIGHEST)
    sign = (2 * core - 1).astype(F32)
    for f in range(2):
        gr, gi = g[2 * f : 2 * f + 1], g[2 * f + 1 : 2 * f + 2]
        wr, wi = tab[4 + 2 * f : 5 + 2 * f, 0:LANES], tab[5 + 2 * f : 6 + 2 * f, 0:LANES]
        same = toeplitz(jnp.concatenate([gr, wr * gr - wi * gi], axis=1))
        cross = toeplitz(jnp.concatenate([gi, wr * gi + wi * gr], axis=1) * sign)
        for r, value in enumerate((same, cross)):
            h, l = halves(value)
            right[f, r * LANES : (r + 1) * LANES, 0:LANES] = h
            right[f, r * LANES : (r + 1) * LANES, LANES : 2 * LANES] = l

    lines[...] = sum(taps[c, pl.ds(4 * e + 2, BLOCKS, stride=8), :] for e in range(2) for c in range(2))

    def block(d, _):
        line = jnp.concatenate([lines[pl.ds(d, 1), :], lines[pl.ds((d + BLOCKS - 1) % BLOCKS, 1), :]], axis=1)
        blocks[d] = toeplitz(line).T
        return 0

    lax.fori_loop(0, BLOCKS, block, 0)

    def block_spectrum(t, _):
        rows = pl.ds(pl.multiple_of(t * 16, 16), 16)
        freqs = rfft([blocks[d, rows, :] for d in range(BLOCKS)])
        zero = jnp.zeros((16, LANES), F32)
        for f in range(8):
            if f == 0:
                quads = ((freqs[0][0], zero), (zero, freqs[8][0]))
            else:
                quads = ((freqs[f][0], -freqs[f][1]), (freqs[f][1], freqs[f][0]))
            for r in range(2):
                for c in range(2):
                    h, l = halves(quads[r][c] * (1.0 / BLOCKS))
                    cols = slice(c * LANES, (c + 1) * LANES)
                    left[f, pl.ds(pl.multiple_of(r * LANES + t * 16, 16), 16), cols] = h
                    left[f, pl.ds(pl.multiple_of(256 + r * LANES + t * 16, 16), 16), cols] = l
        return 0

    lax.fori_loop(0, 8, block_spectrum, 0)

    for f in range(2):
        pltpu.make_async_copy(got.at[f, pl.ds(0, 2016)], got.at[f, pl.ds(0, 2016)], a_recv.at[f]).wait()

        def spectrum(t, _):
            freqs = rfft(
                [got[f, pl.ds(pl.multiple_of(b * LANES + t * 16, 16), 16), :] for b in range(BLOCKS)]
            )
            for k in range(8):
                pair = (freqs[0][0], freqs[8][0]) if k == 0 else freqs[k]
                for r in range(2):
                    h, l = halves(pair[r])
                    rows = pl.ds(pl.multiple_of(r * LANES + t * 16, 16), 16)
                    spec[k, rows, 0:LANES] = h
                    spec[k, rows, LANES : 2 * LANES] = l
            return 0

        lax.fori_loop(0, 8, spectrum, 0, unroll=2)

        def multiply(k, _):
            out = jnp.dot(left[k], spec[k], preferred_element_type=F32)
            out = out[:256] + out[256:]
            prod[k] = out[:, :LANES] + out[:, LANES:]
            return 0

        lax.fori_loop(0, 8, multiply, 0, unroll=2)

        def unspectrum(t, _):
            freqs = []
            for k in range(9):
                re = prod[k % 8, pl.ds(pl.multiple_of((k // 8) * LANES + t * 16, 16), 16), :]
                im = None
                if k % 8:
                    im = prod[k, pl.ds(pl.multiple_of(LANES + t * 16, 16), 16), :]
                freqs.append((re, im))
            for b, value in enumerate(irfft(freqs)):
                done[f, pl.ds(pl.multiple_of(b * LANES + t * 16, 16), 16), :] = value
            return 0

        lax.fori_loop(0, 8, unspectrum, 0, unroll=2)
        swap = remote(done.at[f], other.at[f], swap_send.at[f], swap_recv.at[f], sibling)
        swap.start()
        swap.wait()

        def product(owners):
            rows = [pl.ds(pl.multiple_of(t * 32, 32), 32) for t in owners]
            both = [
                jnp.concatenate([ref[f, r, :] for r in rows], axis=0) for ref in (done, other)
            ]
            h, l = halves(jnp.concatenate(both, axis=1))
            out = jnp.dot(h, right[f], preferred_element_type=F32)
            return out[:, :LANES] + out[:, LANES:] + jnp.dot(l, right[f, :, 0:LANES], preferred_element_type=F32)

        def send_back(owners):
            for to in owners:
                rows = pl.ds(pl.multiple_of(to * 32, 32), 32)
                remote(sent.at[f, rows], back[f].at[:, me, :], b_send.at[f], b_recv.at[f], to).start()

        groups = [peers[j : j + GROUP] for j in range(0, PEERS - 1, GROUP)]
        for j, owners in enumerate(groups):
            out = product(owners)
            for k, to in enumerate(owners):
                sent[f, pl.ds(pl.multiple_of(to * 32, 32), 32), :] = out[k * 32 : (k + 1) * 32]
            if j:
                send_back(groups[j - 1])
        send_back(groups[-1])
        mine = product([me])
        for r in range(32):
            back[f][r, pl.ds(me, 1), :] = mine[r : r + 1]

    small[2].wait()
    small[5].wait()
    down.wait()
    up.wait()
    lane = lax.broadcasted_iota(jnp.int32, (LANES, LANES), 1)

    def stencil_row(y, _):
        total = jnp.zeros((LANES, LANES), F32)
        for a in range(3):
            here = xs[y + a]
            before, after = pltpu.roll(here, 1, 1), pltpu.roll(here, LANES - 1, 1)
            before = jnp.where(lane == 0, pltpu.roll(before, 1, 0), before)
            after = jnp.where(lane == LANES - 1, pltpu.roll(after, LANES - 1, 0), after)
            total = total + stencil[a, 0] * before + stencil[a, 1] * here + stencil[a, 2] * after
        local[y] = total
        return 0

    lax.fori_loop(0, 32, stencil_row, 0)

    for f in range(2):
        pltpu.make_async_copy(got.at[f, pl.ds(0, 2016)], got.at[f, pl.ds(0, 2016)], a_send.at[f]).wait()
    pltpu.make_async_copy(taps.at[0, pl.ds(0, 124)], taps.at[0, pl.ds(0, 124)], tap_send).wait()

    pltpu.make_async_copy(got.at[0, pl.ds(0, 2016)], got.at[0, pl.ds(0, 2016)], b_recv.at[0]).wait()
    add_planes(inv_ref, first, local, local)
    for f in range(2):
        pltpu.make_async_copy(got.at[f, pl.ds(0, 2016)], got.at[f, pl.ds(0, 2016)], b_send.at[f]).wait()
    pltpu.make_async_copy(got.at[1, pl.ds(0, 2016)], got.at[1, pl.ds(0, 2016)], b_recv.at[1]).wait()


def finish(local, last, inv_ref, out_hbm, total, out_sem):
    def store(y):
        pltpu.make_async_copy(total.at[y], out_hbm.at[y // 8, :, y % 8, :], out_sem).start()

    for part in range(PARTS):
        rows = pl.ds(part * 32 // PARTS, 32 // PARTS)
        add_planes(inv_ref, last.at[rows], local.at[rows], total.at[rows])
        for y in range(part * 32 // PARTS, (part + 1) * 32 // PARTS):
            store(y)
    pltpu.make_async_copy(total, total, out_sem).wait()


def tiles(image):
    return image.reshape(4, 8, LANES, LANES).transpose(0, 2, 1, 3)


def body(pixels, row_taps, column_taps, stencil):
    fwd, inv = plane_tables()
    hbm, vmem = pl.BlockSpec(memory_space=pltpu.HBM), pl.BlockSpec(memory_space=pltpu.VMEM)
    block = (32, LANES, LANES)
    half = (32, PEERS, LANES)
    columns = (2, 2048, LANES)
    dma = pltpu.SemaphoreType.DMA
    operands = (
        tiles(pixels), row_taps, column_taps, stencil,
        jnp.asarray(tap_tables()), jnp.asarray(fwd), jnp.asarray(inv[0]),
    )
    local, last = pl.pallas_call(
        kernel,
        out_shape=(pltpu.VMEM(block, F32), pltpu.VMEM(half, F32)),
        in_specs=[hbm] * 7,
        out_specs=(vmem, vmem),
        scratch_shapes=[
            pltpu.VMEM((256,), F32),
            pltpu.VMEM((32,), F32),
            pltpu.SMEM((3, 3), F32),
            pltpu.VMEM((256, 256), BF16),
            pltpu.VMEM((LANES, 192), BF16),
            pltpu.VMEM((8, 2 * LANES), F32),
            pltpu.VMEM((4, LANES), F32),
            pltpu.VMEM((2, LANES, LANES), F32),
            pltpu.VMEM((34, LANES, LANES), F32),
            pltpu.VMEM((2, 32, PEERS, LANES), F32),
            pltpu.VMEM(columns, F32),
            pltpu.VMEM(columns, F32),
            pltpu.VMEM(columns, F32),
            pltpu.VMEM(columns, F32),
            pltpu.VMEM(half, F32),
            pltpu.VMEM((BLOCKS, LANES), F32),
            pltpu.VMEM((BLOCKS, LANES, LANES), F32),
            pltpu.VMEM((8, 512, 256), BF16),
            pltpu.VMEM((8, 256, 256), BF16),
            pltpu.VMEM((8, 256, LANES), F32),
            pltpu.VMEM((2, 256, 256), BF16),
            dma, dma((6,)), dma, dma, dma, dma, dma((2,)), dma((2,)),
            dma((2,)), dma((2,)), dma((2,)), dma((2,)), dma((2,)), dma((2,)),
        ],
        compiler_params=pltpu.CompilerParams(
            collective_id=0, has_side_effects=True, vmem_limit_bytes=MAIN_LIMIT
        ),
        name="filter_rows_and_columns",
    )(*(pltpu.with_memory_space_constraint(operand, pltpu.HBM) for operand in operands))
    out = pl.pallas_call(
        finish,
        out_shape=jax.ShapeDtypeStruct((4, LANES, 8, LANES), F32),
        in_specs=[vmem] * 3,
        out_specs=hbm,
        scratch_shapes=[pltpu.VMEM(block, F32), dma],
        compiler_params=pltpu.CompilerParams(vmem_limit_bytes=FINISH_LIMIT),
        name="last_planes",
    )(local, last, jnp.asarray(inv[1]))
    return out.transpose(0, 2, 1, 3).reshape(pixels.shape)


def solution(mesh):
    in_specs = (
        P(("chan", "rows"), None),
        P(("chan", "rows")),
        P(("chan", "rows")),
        P("chan", None),
    )
    return jax.shard_map(
        body, mesh=mesh, in_specs=in_specs, out_specs=P(("chan", "rows"), None), check_vma=False
    )
```

```python
import math

import jax
import jax.numpy as jnp
import ml_dtypes
import numpy as np
from jax import lax
from jax.experimental import pallas as pl
from jax.experimental.pallas import tpu as pltpu
from jax.sharding import PartitionSpec as P

MESH = pl.DeviceIdType.MESH
F32, BF16 = jnp.float32, jnp.bfloat16
PEERS = 64
LANES = 128
BLOCKS = 16
MAIN_LIMIT = 48 * 2**20
FINISH_LIMIT = 32 * 2**20
PARTS = 4
EDGE = 8
GROUP = 7


STEPS = [
    52, 1, 53, 33, 21, 3, 55, 8, 61, 32, 20, 6, 50, 9, 60, 2,
    54, 25, 44, 7, 51, 24, 45, 35, 23, 30, 43, 27, 47, 5, 49, 11,
    63, 34, 22, 15, 58, 41, 28, 16, 36, 31, 42, 17, 37, 56, 12, 14,
    59, 26, 46, 38, 19, 57, 13, 39, 18, 10, 62, 40, 29, 4, 48,
]


def split_np(values):
    high = values.astype(ml_dtypes.bfloat16)
    low = (values - high.astype(np.float64)).astype(ml_dtypes.bfloat16)
    return high, low


def frequency(device, phase):
    return LANES // 2 if device == 1 and phase == 0 else 2 * (device // 2) + phase


def plane_tables():
    pos = np.arange(LANES)
    fwd = np.zeros((2, PEERS, LANES))
    inv = np.zeros((2, LANES, PEERS))
    for phase in range(2):
        for device in range(PEERS):
            freq = frequency(device, phase)
            angle = 2 * np.pi * (pos * freq % LANES) / LANES
            real = freq in (0, LANES // 2)
            wave = -np.sin(angle) if device % 2 and not real else np.cos(angle)
            fwd[phase, device] = wave
            inv[phase, :, device] = wave * (1 if real else 2) / LANES
    high, low = split_np(fwd.reshape(LANES, LANES))
    forward = np.block([[high, high], [low, low]])
    high, low = split_np(inv)
    return forward, np.concatenate([high, high, low], axis=2)


def tap_tables():
    tab = np.zeros((PEERS, 8, 2 * LANES), np.float64)
    pos = np.arange(LANES)
    cols = pos // 2 % 2 * LANES + pos // 4 * 4 + pos % 2
    for device in range(PEERS):
        for phase in range(2):
            freq = frequency(device, phase)
            angle = 2 * np.pi * (pos * freq % LANES) / LANES
            tab[device, 2 * phase, cols], tab[device, 2 * phase + 1, cols] = np.cos(angle), -np.sin(angle)
            turn = 2 * np.pi * freq / LANES
            tab[device, 4 + 2 * phase], tab[device, 5 + 2 * phase] = np.cos(turn), -np.sin(turn)
    return tab.astype(np.float32)


def turned(k, n, re, im, sign):
    angle = 2 * math.pi * k / n
    c, s = math.cos(angle), sign * math.sin(angle)
    if k == 0:
        return re, im
    if 4 * k == n:
        return (-im, re) if sign > 0 else (im, -re)
    if 8 * k == n:
        return (re - s / abs(s) * im) * c, (im + s / abs(s) * re) * c
    return re * c - im * s, re * s + im * c


def rfft(values):
    n = len(values)
    if n == 2:
        return [(values[0] + values[1], None), (values[0] - values[1], None)]
    even, odd = rfft(values[0::2]), rfft(values[1::2])
    out = [None] * (n // 2 + 1)
    for k in range(n // 4 + 1):
        er, ei = even[k]
        orr, oi = odd[k]
        if k == 0:
            out[0], out[n // 2] = (er + orr, None), (er - orr, None)
        elif 4 * k == n:
            out[k] = (er, -orr)
        else:
            tr, ti = turned(k, n, orr, oi, -1)
            out[k] = (er + tr, ei + ti)
            out[n // 2 - k] = (er - tr, ti - ei)
    return out


def irfft(spectrum):
    n = 2 * (len(spectrum) - 1)
    if n == 2:
        a, b = spectrum[0][0], spectrum[1][0]
        return [a + b, a - b]
    even, odd = [None] * (n // 4 + 1), [None] * (n // 4 + 1)
    for k in range(n // 4 + 1):
        ar, ai = spectrum[k]
        br, bi = spectrum[n // 2 - k]
        if k == 0:
            even[0], odd[0] = (ar + br, None), (ar - br, None)
        elif 4 * k == n:
            even[k], odd[k] = (2.0 * ar, None), (-2.0 * ai, None)
        else:
            even[k] = (ar + br, ai - bi)
            odd[k] = turned(k, n, ar - br, ai + bi, +1)
    out = [None] * n
    out[0::2], out[1::2] = irfft(even), irfft(odd)
    return out


def halves(value):
    high = value.astype(BF16)
    return high, (value - high.astype(F32)).astype(BF16)


def toeplitz(line):
    wide = jnp.broadcast_to(line, (LANES, 2 * LANES))
    return pltpu.roll(wide, 0, 1, stride=1, stride_axis=0)[:, :LANES]


def add_planes(table_ref, planes, base, total):
    def step(i, _):
        h, l = halves(jnp.concatenate([planes[2 * i], planes[2 * i + 1]], axis=1))
        out = jnp.dot(table_ref[...], jnp.concatenate([h, l, h], axis=0), preferred_element_type=F32)
        for r in range(2):
            part = out[:, r * LANES : (r + 1) * LANES]
            total[2 * i + r] = part if base is None else base[2 * i + r] + part
        return 0

    lax.fori_loop(0, total.shape[0] // 2, step, 0, unroll=4)


def kernel(
    x_hbm, row_taps_hbm, col_taps_hbm, stencil_hbm, tab_hbm, fwd_hbm, inv_hbm, local, last,
    row_taps, col_taps, stencil, fwd_ref, inv_ref, tab, my_taps, taps,
    xs, planes, got, raw, done, other, sent, first, lines, blocks, left, spec, prod, right,
    in_sem, small_sems, tap_send, tap_recv, share_send, share_recv,
    a_send, a_recv, swap_send, swap_recv, b_send, b_recv,
):
    me = lax.axis_index("rows")
    core, chip = me % 2, me // 2
    back = (first, last)
    sibling = chip * 2 + 1 - core

    for y in range(32):
        pltpu.make_async_copy(x_hbm.at[y // 8, :, y % 8, :], xs.at[y], in_sem).start()
    pairs = (
        (row_taps_hbm, row_taps), (col_taps_hbm, col_taps), (stencil_hbm, stencil), (fwd_hbm, fwd_ref),
        (tab_hbm.at[me], tab), (inv_hbm, inv_ref),
    )
    small = [pltpu.make_async_copy(src, dst, small_sems.at[i]) for i, (src, dst) in enumerate(pairs)]
    for copy in small:
        copy.start()

    barrier = pltpu.get_barrier_semaphore()

    ys = [(me // 32 + k) % 2 * 32 for k in range(2)]
    xs_at = [(me // 8 + k) % 4 * 8 for k in range(4)]
    zs = [(me // 2 + k) % 4 * 2 for k in range(4)]
    cores = [(me + k) % 2 for k in range(2)]
    peers = [ys[k // 32] + xs_at[k // 8 % 4] + zs[k // 2 % 4] + cores[k % 2] for k in STEPS]

    for to in peers:
        pl.semaphore_signal(barrier, inc=1, device_id={"rows": to}, device_id_type=MESH)

    small[0].wait()
    small[1].wait()
    my_taps[0:1, :] = row_taps[0:128].reshape(1, LANES)
    my_taps[1:2, :] = row_taps[128:256].reshape(1, LANES)
    padded = jnp.concatenate([col_taps[...].reshape(1, 32), jnp.zeros((1, 96), F32)], axis=1)
    my_taps[2:3, :] = pltpu.roll(padded, (me % 4) * 32, 1)
    my_taps[3:4, :] = jnp.zeros((1, LANES), F32)
    my_tap_rows = pl.ds(pl.multiple_of(chip * 4, 4), 4)
    taps[core, my_tap_rows, :] = my_taps[...]

    small[3].wait()

    def to_planes(i, _):
        pair = jnp.concatenate([xs[2 * i], xs[2 * i + 1]], axis=1)
        out = jnp.dot(fwd_ref[...], jnp.concatenate(halves(pair), axis=0), preferred_element_type=F32)
        out = out[:LANES] + out[LANES:]
        for f in range(2):
            for r in range(2):
                planes[f, 2 * i + r] = out[f * PEERS : (f + 1) * PEERS, r * LANES : (r + 1) * LANES]
        return 0

    pltpu.make_async_copy(xs, xs, in_sem).wait()
    lax.fori_loop(0, 16, to_planes, 0, unroll=16)
    pl.semaphore_wait(barrier, PEERS - 1)

    def remote(src, dst, send, recv, to):
        return pltpu.make_async_remote_copy(
            src_ref=src, dst_ref=dst, send_sem=send, recv_sem=recv, device_id={"rows": to}, device_id_type=MESH
        )

    for step, to in zip(STEPS, peers):
        if step % 2 == 0:
            remote(my_taps, taps.at[core, my_tap_rows, :], tap_send, tap_recv, to).start()
    for f in range(2):
        for to in peers:
            remote(
                planes.at[f, :, to, :],
                got.at[f, pl.ds(pl.multiple_of(me * 32 + EDGE, EDGE), 32)],
                a_send.at[f],
                a_recv.at[f],
                to,
            ).start()

    for f in range(2):

        def own(r, _):
            got[f, pl.ds(me * 32 + EDGE + r, 1), :] = planes[f, r, pl.ds(me, 1), :]
            return 0

        lax.fori_loop(0, 32, own, 0)

    small[4].wait()
    pltpu.make_async_copy(taps.at[0, pl.ds(0, 124)], taps.at[0, pl.ds(0, 124)], tap_recv).wait()
    share = remote(taps.at[core], taps.at[core], share_send, share_recv, sibling)
    share.start()
    share.wait()
    g = jnp.dot(tab[:, 0:LANES], taps[0], preferred_element_type=F32, precision=lax.Precision.HIGHEST)
    g = g + jnp.dot(tab[:, LANES:], taps[1], preferred_element_type=F32, precision=lax.Precision.HIGHEST)
    sign = (2 * core - 1).astype(F32)
    small[2].wait()
    lane = lax.broadcasted_iota(jnp.int32, (1, LANES), 1)
    for f in range(2):
        wr, wi = tab[4 + 2 * f : 5 + 2 * f, 0:LANES], tab[5 + 2 * f : 6 + 2 * f, 0:LANES]
        lines_of = [(g[2 * f : 2 * f + 1], g[2 * f + 1 : 2 * f + 2])]
        for a in range(3):
            ahead = jnp.where(lane == LANES - 1, stencil[a, 2], 0.0)
            here = jnp.where(lane == 0, stencil[a, 1], 0.0) + jnp.where(lane == 1, stencil[a, 0], 0.0)
            lines_of.append((here + ahead * wr, -ahead * wi))
        for part, (gr, gi) in enumerate(lines_of):
            same = toeplitz(jnp.concatenate([gr, wr * gr - wi * gi], axis=1))
            cross = toeplitz(jnp.concatenate([gi, wr * gi + wi * gr], axis=1) * sign)
            for r, value in enumerate((same, cross)):
                h, l = halves(value)
                at = (2 * part + r) * LANES
                right[f, at : at + LANES, 0:LANES] = h
                right[f, at : at + LANES, LANES : 2 * LANES] = l

    lines[...] = sum(taps[c, pl.ds(4 * e + 2, BLOCKS, stride=8), :] for e in range(2) for c in range(2))

    def block(d, _):
        line = jnp.concatenate([lines[pl.ds(d, 1), :], lines[pl.ds((d + BLOCKS - 1) % BLOCKS, 1), :]], axis=1)
        blocks[d] = toeplitz(line).T
        return 0

    lax.fori_loop(0, BLOCKS, block, 0)

    def block_spectrum(t, _):
        rows = pl.ds(pl.multiple_of(t * 16, 16), 16)
        freqs = rfft([blocks[d, rows, :] for d in range(BLOCKS)])
        zero = jnp.zeros((16, LANES), F32)
        for f in range(8):
            if f == 0:
                quads = ((freqs[0][0], zero), (zero, freqs[8][0]))
            else:
                quads = ((freqs[f][0], -freqs[f][1]), (freqs[f][1], freqs[f][0]))
            for r in range(2):
                for c in range(2):
                    h, l = halves(quads[r][c] * (1.0 / BLOCKS))
                    cols = slice(c * LANES, (c + 1) * LANES)
                    left[f, pl.ds(pl.multiple_of(r * LANES + t * 16, 16), 16), cols] = h
                    left[f, pl.ds(pl.multiple_of(256 + r * LANES + t * 16, 16), 16), cols] = l
        return 0

    lax.fori_loop(0, 8, block_spectrum, 0)

    for f in range(2):
        pltpu.make_async_copy(got.at[f, pl.ds(0, 2016)], got.at[f, pl.ds(0, 2016)], a_recv.at[f]).wait()

        def spectrum(t, _):
            freqs = rfft(
                [got[f, pl.ds(pl.multiple_of(b * LANES + t * 16 + EDGE, EDGE), 16), :] for b in range(BLOCKS)]
            )
            for k in range(8):
                pair = (freqs[0][0], freqs[8][0]) if k == 0 else freqs[k]
                for r in range(2):
                    h, l = halves(pair[r])
                    rows = pl.ds(pl.multiple_of(r * LANES + t * 16, 16), 16)
                    spec[k, rows, 0:LANES] = h
                    spec[k, rows, LANES : 2 * LANES] = l
            return 0

        got[f, 0:EDGE, :] = got[f, 2048 : 2048 + EDGE, :]
        got[f, 2048 + EDGE : 2048 + 2 * EDGE, :] = got[f, EDGE : 2 * EDGE, :]
        lax.fori_loop(0, 8, spectrum, 0, unroll=2)
        share_raw = remote(got.at[f], raw.at[f], swap_send.at[2 + f], swap_recv.at[2 + f], sibling)
        share_raw.start()

        def multiply(k, _):
            out = jnp.dot(left[k], spec[k], preferred_element_type=F32)
            out = out[:256] + out[256:]
            prod[k] = out[:, :LANES] + out[:, LANES:]
            return 0

        lax.fori_loop(0, 8, multiply, 0, unroll=2)

        def unspectrum(t, _):
            freqs = []
            for k in range(9):
                re = prod[k % 8, pl.ds(pl.multiple_of((k // 8) * LANES + t * 16, 16), 16), :]
                im = None
                if k % 8:
                    im = prod[k, pl.ds(pl.multiple_of(LANES + t * 16, 16), 16), :]
                freqs.append((re, im))
            for b, value in enumerate(irfft(freqs)):
                done[f, pl.ds(pl.multiple_of(b * LANES + t * 16, 16), 16), :] = value
            return 0

        lax.fori_loop(0, 8, unspectrum, 0, unroll=2)
        swap = remote(done.at[f], other.at[f], swap_send.at[f], swap_recv.at[f], sibling)
        swap.start()
        share_raw.wait()
        swap.wait()

        def product(owners):
            rows = [pl.ds(pl.multiple_of(t * 32, 32), 32) for t in owners]
            parts = [jnp.concatenate([ref[f, r, :] for r in rows], axis=0) for ref in (done, other)]
            near = [
                [ref[f, pl.ds(pl.multiple_of(t * 32, 32), 32 + 2 * EDGE), :] for t in owners] for ref in (got, raw)
            ]
            for a in range(3):
                first_row = EDGE - 1 + a
                parts += [jnp.concatenate([v[first_row : first_row + 32] for v in vs], axis=0) for vs in near]
            h, l = halves(jnp.concatenate(parts, axis=1))
            out = jnp.dot(h, right[f], preferred_element_type=F32)
            return out[:, :LANES] + out[:, LANES:] + jnp.dot(l, right[f, :, 0:LANES], preferred_element_type=F32)

        def send_back(owners):
            for to in owners:
                rows = pl.ds(pl.multiple_of(to * 32, 32), 32)
                remote(sent.at[f, rows], back[f].at[:, me, :], b_send.at[f], b_recv.at[f], to).start()

        groups = [peers[j : j + GROUP] for j in range(0, PEERS - 1, GROUP)]
        for j, owners in enumerate(groups):
            out = product(owners)
            for k, to in enumerate(owners):
                sent[f, pl.ds(pl.multiple_of(to * 32, 32), 32), :] = out[k * 32 : (k + 1) * 32]
            if j:
                send_back(groups[j - 1])
        send_back(groups[-1])
        mine = product([me])
        for r in range(32):
            back[f][r, pl.ds(me, 1), :] = mine[r : r + 1]

    small[5].wait()
    for f in range(2):
        pltpu.make_async_copy(got.at[f, pl.ds(0, 2016)], got.at[f, pl.ds(0, 2016)], a_send.at[f]).wait()
    pltpu.make_async_copy(taps.at[0, pl.ds(0, 124)], taps.at[0, pl.ds(0, 124)], tap_send).wait()

    pltpu.make_async_copy(got.at[0, pl.ds(0, 2016)], got.at[0, pl.ds(0, 2016)], b_recv.at[0]).wait()
    add_planes(inv_ref, first, None, local)
    for f in range(2):
        pltpu.make_async_copy(got.at[f, pl.ds(0, 2016)], got.at[f, pl.ds(0, 2016)], b_send.at[f]).wait()
    pltpu.make_async_copy(got.at[1, pl.ds(0, 2016)], got.at[1, pl.ds(0, 2016)], b_recv.at[1]).wait()


def finish(local, last, inv_ref, out_hbm, total, out_sem):
    def store(y):
        pltpu.make_async_copy(total.at[y], out_hbm.at[y // 8, :, y % 8, :], out_sem).start()

    for part in range(PARTS):
        rows = pl.ds(part * 32 // PARTS, 32 // PARTS)
        add_planes(inv_ref, last.at[rows], local.at[rows], total.at[rows])
        for y in range(part * 32 // PARTS, (part + 1) * 32 // PARTS):
            store(y)
    pltpu.make_async_copy(total, total, out_sem).wait()


def tiles(image):
    return image.reshape(4, 8, LANES, LANES).transpose(0, 2, 1, 3)


def body(pixels, row_taps, column_taps, stencil):
    fwd, inv = plane_tables()
    hbm, vmem = pl.BlockSpec(memory_space=pltpu.HBM), pl.BlockSpec(memory_space=pltpu.VMEM)
    block = (32, LANES, LANES)
    half = (32, PEERS, LANES)
    columns, edged = (2, 2048, LANES), (2, 2048 + 2 * EDGE, LANES)
    dma = pltpu.SemaphoreType.DMA
    operands = (
        tiles(pixels), row_taps, column_taps, stencil,
        jnp.asarray(tap_tables()), jnp.asarray(fwd), jnp.asarray(inv[0]),
    )
    local, last = pl.pallas_call(
        kernel,
        out_shape=(pltpu.VMEM(block, F32), pltpu.VMEM(half, F32)),
        in_specs=[hbm] * 7,
        out_specs=(vmem, vmem),
        scratch_shapes=[
            pltpu.VMEM((256,), F32),
            pltpu.VMEM((32,), F32),
            pltpu.SMEM((3, 3), F32),
            pltpu.VMEM((256, 256), BF16),
            pltpu.VMEM((LANES, 192), BF16),
            pltpu.VMEM((8, 2 * LANES), F32),
            pltpu.VMEM((4, LANES), F32),
            pltpu.VMEM((2, LANES, LANES), F32),
            pltpu.VMEM(block, F32),
            pltpu.VMEM((2, 32, PEERS, LANES), F32),
            pltpu.VMEM(edged, F32),
            pltpu.VMEM(edged, F32),
            pltpu.VMEM(columns, F32),
            pltpu.VMEM(columns, F32),
            pltpu.VMEM(columns, F32),
            pltpu.VMEM(half, F32),
            pltpu.VMEM((BLOCKS, LANES), F32),
            pltpu.VMEM((BLOCKS, LANES, LANES), F32),
            pltpu.VMEM((8, 512, 256), BF16),
            pltpu.VMEM((8, 256, 256), BF16),
            pltpu.VMEM((8, 256, LANES), F32),
            pltpu.VMEM((2, 1024, 256), BF16),
            dma, dma((6,)), dma, dma, dma, dma,
            dma((2,)), dma((2,)), dma((4,)), dma((4,)), dma((2,)), dma((2,)),
        ],
        compiler_params=pltpu.CompilerParams(
            collective_id=0, has_side_effects=True, vmem_limit_bytes=MAIN_LIMIT
        ),
        name="filter_rows_and_columns",
    )(*(pltpu.with_memory_space_constraint(operand, pltpu.HBM) for operand in operands))
    out = pl.pallas_call(
        finish,
        out_shape=jax.ShapeDtypeStruct((4, LANES, 8, LANES), F32),
        in_specs=[vmem] * 3,
        out_specs=hbm,
        scratch_shapes=[pltpu.VMEM(block, F32), dma],
        compiler_params=pltpu.CompilerParams(vmem_limit_bytes=FINISH_LIMIT),
        name="last_planes",
    )(local, last, jnp.asarray(inv[1]))
    return out.transpose(0, 2, 1, 3).reshape(pixels.shape)


def solution(mesh):
    in_specs = (
        P(("chan", "rows"), None),
        P(("chan", "rows")),
        P(("chan", "rows")),
        P("chan", None),
    )
    return jax.shard_map(
        body, mesh=mesh, in_specs=in_specs, out_specs=P(("chan", "rows"), None), check_vma=False
    )
```

```python
import math

import jax
import jax.numpy as jnp
import ml_dtypes
import numpy as np
from jax import lax
from jax.experimental import pallas as pl
from jax.experimental.pallas import tpu as pltpu
from jax.sharding import PartitionSpec as P

MESH = pl.DeviceIdType.MESH
F32, BF16 = jnp.float32, jnp.bfloat16
PEERS = 64
LANES = 128
BLOCKS = 16
MAIN_LIMIT = 48 * 2**20
FINISH_LIMIT = 32 * 2**20
PARTS = 4
EDGE = 8
GROUP = 7


STEPS = [
    52, 1, 53, 24, 44, 7, 51, 25, 45, 3, 54, 32, 20, 33, 21, 6,
    50, 2, 55, 8, 61, 9, 60, 34, 22, 38, 18, 56, 12, 11, 63, 35,
    23, 4, 49, 26, 46, 30, 42, 5, 48, 27, 47, 41, 29, 57, 13, 14,
    59, 16, 37, 31, 43, 40, 28, 10, 62, 17, 36, 39, 19, 15, 58,
]


def split_np(values):
    high = values.astype(ml_dtypes.bfloat16)
    low = (values - high.astype(np.float64)).astype(ml_dtypes.bfloat16)
    return high, low


def frequency(device, phase):
    return LANES // 2 if device == 1 and phase == 0 else 2 * (device // 2) + phase


def plane_tables():
    pos = np.arange(LANES)
    fwd = np.zeros((2, PEERS, LANES))
    inv = np.zeros((2, LANES, PEERS))
    for phase in range(2):
        for device in range(PEERS):
            freq = frequency(device, phase)
            angle = 2 * np.pi * (pos * freq % LANES) / LANES
            real = freq in (0, LANES // 2)
            wave = -np.sin(angle) if device % 2 and not real else np.cos(angle)
            fwd[phase, device] = wave
            inv[phase, :, device] = wave * (1 if real else 2) / LANES
    high, low = split_np(fwd.reshape(LANES, LANES))
    forward = np.block([[high, high], [low, low]])
    high, low = split_np(inv)
    return forward, np.concatenate([high, high, low], axis=2)


def tap_tables():
    tab = np.zeros((PEERS, 8, 2 * LANES), np.float64)
    pos = np.arange(LANES)
    cols = pos // 2 % 2 * LANES + pos // 4 * 4 + pos % 2
    for device in range(PEERS):
        for phase in range(2):
            freq = frequency(device, phase)
            angle = 2 * np.pi * (pos * freq % LANES) / LANES
            tab[device, 2 * phase, cols], tab[device, 2 * phase + 1, cols] = np.cos(angle), -np.sin(angle)
            turn = 2 * np.pi * freq / LANES
            tab[device, 4 + 2 * phase], tab[device, 5 + 2 * phase] = np.cos(turn), -np.sin(turn)
    return tab.astype(np.float32)


def turned(k, n, re, im, sign):
    angle = 2 * math.pi * k / n
    c, s = math.cos(angle), sign * math.sin(angle)
    if k == 0:
        return re, im
    if 4 * k == n:
        return (-im, re) if sign > 0 else (im, -re)
    if 8 * k == n:
        return (re - s / abs(s) * im) * c, (im + s / abs(s) * re) * c
    return re * c - im * s, re * s + im * c


def rfft(values):
    n = len(values)
    if n == 2:
        return [(values[0] + values[1], None), (values[0] - values[1], None)]
    even, odd = rfft(values[0::2]), rfft(values[1::2])
    out = [None] * (n // 2 + 1)
    for k in range(n // 4 + 1):
        er, ei = even[k]
        orr, oi = odd[k]
        if k == 0:
            out[0], out[n // 2] = (er + orr, None), (er - orr, None)
        elif 4 * k == n:
            out[k] = (er, -orr)
        else:
            tr, ti = turned(k, n, orr, oi, -1)
            out[k] = (er + tr, ei + ti)
            out[n // 2 - k] = (er - tr, ti - ei)
    return out


def irfft(spectrum):
    n = 2 * (len(spectrum) - 1)
    if n == 2:
        a, b = spectrum[0][0], spectrum[1][0]
        return [a + b, a - b]
    even, odd = [None] * (n // 4 + 1), [None] * (n // 4 + 1)
    for k in range(n // 4 + 1):
        ar, ai = spectrum[k]
        br, bi = spectrum[n // 2 - k]
        if k == 0:
            even[0], odd[0] = (ar + br, None), (ar - br, None)
        elif 4 * k == n:
            even[k], odd[k] = (2.0 * ar, None), (-2.0 * ai, None)
        else:
            even[k] = (ar + br, ai - bi)
            odd[k] = turned(k, n, ar - br, ai + bi, +1)
    out = [None] * n
    out[0::2], out[1::2] = irfft(even), irfft(odd)
    return out


def halves(value):
    high = value.astype(BF16)
    return high, (value - high.astype(F32)).astype(BF16)


def toeplitz(line):
    wide = jnp.broadcast_to(line, (LANES, 2 * LANES))
    return pltpu.roll(wide, 0, 1, stride=1, stride_axis=0)[:, :LANES]


def add_planes(table_ref, planes, base, total):
    def step(i, _):
        h, l = halves(jnp.concatenate([planes[2 * i], planes[2 * i + 1]], axis=1))
        out = jnp.dot(table_ref[...], jnp.concatenate([h, l, h], axis=0), preferred_element_type=F32)
        for r in range(2):
            part = out[:, r * LANES : (r + 1) * LANES]
            total[2 * i + r] = part if base is None else base[2 * i + r] + part
        return 0

    lax.fori_loop(0, total.shape[0] // 2, step, 0, unroll=4)


def kernel(
    x_hbm, row_taps_hbm, col_taps_hbm, stencil_hbm, tab_hbm, fwd_hbm, inv_hbm, local, last,
    row_taps, col_taps, stencil, fwd_ref, inv_ref, tab, my_taps, taps,
    xs, planes, got, raw, done, other, sent, first, lines, blocks, left, spec, prod, right,
    in_sem, small_sems, tap_send, tap_recv, share_send, share_recv,
    a_send, a_recv, swap_send, swap_recv, b_send, b_recv,
):
    me = lax.axis_index("rows")
    core, chip = me % 2, me // 2
    back = (first, last)
    sibling = chip * 2 + 1 - core

    for y in range(32):
        pltpu.make_async_copy(x_hbm.at[y // 8, :, y % 8, :], xs.at[y], in_sem).start()
    pairs = (
        (row_taps_hbm, row_taps), (col_taps_hbm, col_taps), (stencil_hbm, stencil), (fwd_hbm, fwd_ref),
        (tab_hbm.at[me], tab), (inv_hbm, inv_ref),
    )
    small = [pltpu.make_async_copy(src, dst, small_sems.at[i]) for i, (src, dst) in enumerate(pairs)]
    for copy in small:
        copy.start()

    barrier = pltpu.get_barrier_semaphore()

    ys = [(me // 32 + k) % 2 * 32 for k in range(2)]
    xs_at = [(me // 8 + k) % 4 * 8 for k in range(4)]
    zs = [(me // 2 + k) % 4 * 2 for k in range(4)]
    cores = [(me + k) % 2 for k in range(2)]
    peers = [ys[k // 32] + xs_at[k // 8 % 4] + zs[k // 2 % 4] + cores[k % 2] for k in STEPS]

    for to in peers:
        pl.semaphore_signal(barrier, inc=1, device_id={"rows": to}, device_id_type=MESH)

    small[0].wait()
    small[1].wait()
    my_taps[0:1, :] = row_taps[0:128].reshape(1, LANES)
    my_taps[1:2, :] = row_taps[128:256].reshape(1, LANES)
    padded = jnp.concatenate([col_taps[...].reshape(1, 32), jnp.zeros((1, 96), F32)], axis=1)
    my_taps[2:3, :] = pltpu.roll(padded, (me % 4) * 32, 1)
    my_taps[3:4, :] = jnp.zeros((1, LANES), F32)
    my_tap_rows = pl.ds(pl.multiple_of(chip * 4, 4), 4)
    taps[core, my_tap_rows, :] = my_taps[...]

    small[3].wait()

    def to_planes(i, _):
        pair = jnp.concatenate([xs[2 * i], xs[2 * i + 1]], axis=1)
        out = jnp.dot(fwd_ref[...], jnp.concatenate(halves(pair), axis=0), preferred_element_type=F32)
        out = out[:LANES] + out[LANES:]
        for f in range(2):
            for r in range(2):
                planes[f, 2 * i + r] = out[f * PEERS : (f + 1) * PEERS, r * LANES : (r + 1) * LANES]
        return 0

    pltpu.make_async_copy(xs, xs, in_sem).wait()
    lax.fori_loop(0, 16, to_planes, 0, unroll=16)
    pl.semaphore_wait(barrier, PEERS - 1)

    def remote(src, dst, send, recv, to):
        return pltpu.make_async_remote_copy(
            src_ref=src, dst_ref=dst, send_sem=send, recv_sem=recv, device_id={"rows": to}, device_id_type=MESH
        )

    for step, to in zip(STEPS, peers):
        if step % 2 == 0:
            remote(my_taps, taps.at[core, my_tap_rows, :], tap_send, tap_recv, to).start()
    for f in range(2):
        for to in peers:
            remote(
                planes.at[f, :, to, :],
                got.at[f, pl.ds(pl.multiple_of(me * 32 + EDGE, EDGE), 32)],
                a_send.at[f],
                a_recv.at[f],
                to,
            ).start()

    for f in range(2):

        def own(r, _):
            got[f, pl.ds(me * 32 + EDGE + r, 1), :] = planes[f, r, pl.ds(me, 1), :]
            return 0

        lax.fori_loop(0, 32, own, 0)

    small[4].wait()
    pltpu.make_async_copy(taps.at[0, pl.ds(0, 124)], taps.at[0, pl.ds(0, 124)], tap_recv).wait()
    share = remote(taps.at[core], taps.at[core], share_send, share_recv, sibling)
    share.start()
    share.wait()
    g = jnp.dot(tab[:, 0:LANES], taps[0], preferred_element_type=F32, precision=lax.Precision.HIGHEST)
    g = g + jnp.dot(tab[:, LANES:], taps[1], preferred_element_type=F32, precision=lax.Precision.HIGHEST)
    sign = (2 * core - 1).astype(F32)
    small[2].wait()
    lane = lax.broadcasted_iota(jnp.int32, (1, LANES), 1)
    for f in range(2):
        wr, wi = tab[4 + 2 * f : 5 + 2 * f, 0:LANES], tab[5 + 2 * f : 6 + 2 * f, 0:LANES]
        lines_of = [(g[2 * f : 2 * f + 1], g[2 * f + 1 : 2 * f + 2])]
        for a in range(3):
            ahead = jnp.where(lane == LANES - 1, stencil[a, 2], 0.0)
            here = jnp.where(lane == 0, stencil[a, 1], 0.0) + jnp.where(lane == 1, stencil[a, 0], 0.0)
            lines_of.append((here + ahead * wr, -ahead * wi))
        for part, (gr, gi) in enumerate(lines_of):
            same = toeplitz(jnp.concatenate([gr, wr * gr - wi * gi], axis=1))
            cross = toeplitz(jnp.concatenate([gi, wr * gi + wi * gr], axis=1) * sign)
            for r, value in enumerate((same, cross)):
                h, l = halves(value)
                at = (2 * part + r) * LANES
                right[f, at : at + LANES, 0:LANES] = h
                right[f, at : at + LANES, LANES : 2 * LANES] = l

    lines[...] = sum(taps[c, pl.ds(4 * e + 2, BLOCKS, stride=8), :] for e in range(2) for c in range(2))

    def block(d, _):
        line = jnp.concatenate([lines[pl.ds(d, 1), :], lines[pl.ds((d + BLOCKS - 1) % BLOCKS, 1), :]], axis=1)
        blocks[d] = toeplitz(line).T
        return 0

    lax.fori_loop(0, BLOCKS, block, 0)

    def block_spectrum(t, _):
        rows = pl.ds(pl.multiple_of(t * 16, 16), 16)
        freqs = rfft([blocks[d, rows, :] for d in range(BLOCKS)])
        zero = jnp.zeros((16, LANES), F32)
        for f in range(8):
            if f == 0:
                quads = ((freqs[0][0], zero), (zero, freqs[8][0]))
            else:
                quads = ((freqs[f][0], -freqs[f][1]), (freqs[f][1], freqs[f][0]))
            for r in range(2):
                for c in range(2):
                    h, l = halves(quads[r][c] * (1.0 / BLOCKS))
                    cols = slice(c * LANES, (c + 1) * LANES)
                    left[f, pl.ds(pl.multiple_of(r * LANES + t * 16, 16), 16), cols] = h
                    left[f, pl.ds(pl.multiple_of(256 + r * LANES + t * 16, 16), 16), cols] = l
        return 0

    lax.fori_loop(0, 8, block_spectrum, 0)

    for f in range(2):
        pltpu.make_async_copy(got.at[f, pl.ds(0, 2016)], got.at[f, pl.ds(0, 2016)], a_recv.at[f]).wait()

        def spectrum(t, _):
            freqs = rfft(
                [got[f, pl.ds(pl.multiple_of(b * LANES + t * 16 + EDGE, EDGE), 16), :] for b in range(BLOCKS)]
            )
            for k in range(8):
                pair = (freqs[0][0], freqs[8][0]) if k == 0 else freqs[k]
                for r in range(2):
                    h, l = halves(pair[r])
                    rows = pl.ds(pl.multiple_of(r * LANES + t * 16, 16), 16)
                    spec[k, rows, 0:LANES] = h
                    spec[k, rows, LANES : 2 * LANES] = l
            return 0

        got[f, 0:EDGE, :] = got[f, 2048 : 2048 + EDGE, :]
        got[f, 2048 + EDGE : 2048 + 2 * EDGE, :] = got[f, EDGE : 2 * EDGE, :]
        lax.fori_loop(0, 8, spectrum, 0, unroll=2)
        share_raw = remote(got.at[f], raw.at[f], swap_send.at[2 + f], swap_recv.at[2 + f], sibling)
        share_raw.start()

        def multiply(k, _):
            out = jnp.dot(left[k], spec[k], preferred_element_type=F32)
            out = out[:256] + out[256:]
            prod[k] = out[:, :LANES] + out[:, LANES:]
            return 0

        lax.fori_loop(0, 8, multiply, 0, unroll=2)

        def unspectrum(t, _):
            freqs = []
            for k in range(9):
                re = prod[k % 8, pl.ds(pl.multiple_of((k // 8) * LANES + t * 16, 16), 16), :]
                im = None
                if k % 8:
                    im = prod[k, pl.ds(pl.multiple_of(LANES + t * 16, 16), 16), :]
                freqs.append((re, im))
            for b, value in enumerate(irfft(freqs)):
                done[f, pl.ds(pl.multiple_of(b * LANES + t * 16, 16), 16), :] = value
            return 0

        lax.fori_loop(0, 8, unspectrum, 0, unroll=2)
        swap = remote(done.at[f], other.at[f], swap_send.at[f], swap_recv.at[f], sibling)
        swap.start()
        share_raw.wait()
        swap.wait()

        def product(owners):
            rows = [pl.ds(pl.multiple_of(t * 32, 32), 32) for t in owners]
            parts = [jnp.concatenate([ref[f, r, :] for r in rows], axis=0) for ref in (done, other)]
            near = [
                [ref[f, pl.ds(pl.multiple_of(t * 32, 32), 32 + 2 * EDGE), :] for t in owners] for ref in (got, raw)
            ]
            for a in range(3):
                first_row = EDGE - 1 + a
                parts += [jnp.concatenate([v[first_row : first_row + 32] for v in vs], axis=0) for vs in near]
            h, l = halves(jnp.concatenate(parts, axis=1))
            out = jnp.dot(h, right[f], preferred_element_type=F32)
            return out[:, :LANES] + out[:, LANES:] + jnp.dot(l, right[f, :, 0:LANES], preferred_element_type=F32)

        def send_back(owners):
            for to in owners:
                rows = pl.ds(pl.multiple_of(to * 32, 32), 32)
                remote(sent.at[f, rows], back[f].at[:, me, :], b_send.at[f], b_recv.at[f], to).start()

        groups = [peers[j : j + GROUP] for j in range(0, PEERS - 1, GROUP)]
        for j, owners in enumerate(groups):
            out = product(owners)
            for k, to in enumerate(owners):
                sent[f, pl.ds(pl.multiple_of(to * 32, 32), 32), :] = out[k * 32 : (k + 1) * 32]
            if j:
                send_back(groups[j - 1])
        send_back(groups[-1])
        mine = product([me])
        for r in range(32):
            back[f][r, pl.ds(me, 1), :] = mine[r : r + 1]

    small[5].wait()
    for f in range(2):
        pltpu.make_async_copy(got.at[f, pl.ds(0, 2016)], got.at[f, pl.ds(0, 2016)], a_send.at[f]).wait()
    pltpu.make_async_copy(taps.at[0, pl.ds(0, 124)], taps.at[0, pl.ds(0, 124)], tap_send).wait()

    pltpu.make_async_copy(got.at[0, pl.ds(0, 2016)], got.at[0, pl.ds(0, 2016)], b_recv.at[0]).wait()
    add_planes(inv_ref, first, None, local)
    for f in range(2):
        pltpu.make_async_copy(got.at[f, pl.ds(0, 2016)], got.at[f, pl.ds(0, 2016)], b_send.at[f]).wait()
    pltpu.make_async_copy(got.at[1, pl.ds(0, 2016)], got.at[1, pl.ds(0, 2016)], b_recv.at[1]).wait()


def finish(local, last, inv_ref, out_hbm, total, out_sem):
    def store(y):
        pltpu.make_async_copy(total.at[y], out_hbm.at[y // 8, :, y % 8, :], out_sem).start()

    for part in range(PARTS):
        rows = pl.ds(part * 32 // PARTS, 32 // PARTS)
        add_planes(inv_ref, last.at[rows], local.at[rows], total.at[rows])
        for y in range(part * 32 // PARTS, (part + 1) * 32 // PARTS):
            store(y)
    pltpu.make_async_copy(total, total, out_sem).wait()


def tiles(image):
    return image.reshape(4, 8, LANES, LANES).transpose(0, 2, 1, 3)


def body(pixels, row_taps, column_taps, stencil):
    fwd, inv = plane_tables()
    hbm, vmem = pl.BlockSpec(memory_space=pltpu.HBM), pl.BlockSpec(memory_space=pltpu.VMEM)
    block = (32, LANES, LANES)
    half = (32, PEERS, LANES)
    columns, edged = (2, 2048, LANES), (2, 2048 + 2 * EDGE, LANES)
    dma = pltpu.SemaphoreType.DMA
    operands = (
        tiles(pixels), row_taps, column_taps, stencil,
        jnp.asarray(tap_tables()), jnp.asarray(fwd), jnp.asarray(inv[0]),
    )
    local, last = pl.pallas_call(
        kernel,
        out_shape=(pltpu.VMEM(block, F32), pltpu.VMEM(half, F32)),
        in_specs=[hbm] * 7,
        out_specs=(vmem, vmem),
        scratch_shapes=[
            pltpu.VMEM((256,), F32),
            pltpu.VMEM((32,), F32),
            pltpu.SMEM((3, 3), F32),
            pltpu.VMEM((256, 256), BF16),
            pltpu.VMEM((LANES, 192), BF16),
            pltpu.VMEM((8, 2 * LANES), F32),
            pltpu.VMEM((4, LANES), F32),
            pltpu.VMEM((2, LANES, LANES), F32),
            pltpu.VMEM(block, F32),
            pltpu.VMEM((2, 32, PEERS, LANES), F32),
            pltpu.VMEM(edged, F32),
            pltpu.VMEM(edged, F32),
            pltpu.VMEM(columns, F32),
            pltpu.VMEM(columns, F32),
            pltpu.VMEM(columns, F32),
            pltpu.VMEM(half, F32),
            pltpu.VMEM((BLOCKS, LANES), F32),
            pltpu.VMEM((BLOCKS, LANES, LANES), F32),
            pltpu.VMEM((8, 512, 256), BF16),
            pltpu.VMEM((8, 256, 256), BF16),
            pltpu.VMEM((8, 256, LANES), F32),
            pltpu.VMEM((2, 1024, 256), BF16),
            dma, dma((6,)), dma, dma, dma, dma,
            dma((2,)), dma((2,)), dma((4,)), dma((4,)), dma((2,)), dma((2,)),
        ],
        compiler_params=pltpu.CompilerParams(
            collective_id=0, has_side_effects=True, vmem_limit_bytes=MAIN_LIMIT
        ),
        name="filter_rows_and_columns",
    )(*(pltpu.with_memory_space_constraint(operand, pltpu.HBM) for operand in operands))
    out = pl.pallas_call(
        finish,
        out_shape=jax.ShapeDtypeStruct((4, LANES, 8, LANES), F32),
        in_specs=[vmem] * 3,
        out_specs=hbm,
        scratch_shapes=[pltpu.VMEM(block, F32), dma],
        compiler_params=pltpu.CompilerParams(vmem_limit_bytes=FINISH_LIMIT),
        name="last_planes",
    )(local, last, jnp.asarray(inv[1]))
    return out.transpose(0, 2, 1, 3).reshape(pixels.shape)


def solution(mesh):
    in_specs = (
        P(("chan", "rows"), None),
        P(("chan", "rows")),
        P(("chan", "rows")),
        P("chan", None),
    )
    return jax.shard_map(
        body, mesh=mesh, in_specs=in_specs, out_specs=P(("chan", "rows"), None), check_vma=False
    )
```
